256 devices in a mesh: dom: 128 (over x, z, y), field: 2 (over core).
Axes of the slice: x: 4, y: 4, z: 8, core: 2. Of those that a mesh axis runs over, the one named last changes fastest.
Arguments:
- ocean: bfloat16 [30, 262144], P('field', 'dom'), may hold values from -6 to 6
- grad_weight: bfloat16 [2048, 4, 128, 256], P('dom'), may hold values from -0.25 to 0.25
- neighbours: int32 [2048, 4], P('dom'), may hold values from 0 to 2047, as said below
- remap_weight: bfloat16 [16384, 384, 128], P(('dom', 'field')), may hold values from -0.109375 to 0.109375
- tile_src: int32 [16384], P(('dom', 'field')), may hold values from 0 to 2047, as said below
- tile_atm: int32 [16384], P(('dom', 'field')), may hold values from 0 to 2047, as said below
- atm_owner: int32 [2048], replicated, may hold values from 0 to 2047, as said below
Outputs:
- atmosphere: float32 [30, 262144], P('field', 'dom')
The draws below stay inside these ranges and needn't reach their ends.
Inputs may be any that keep to these rules, and one draw needn't show every extreme that they name: `neighbours`: the stencil of a block of partition p holds blocks of p, the last 2 blocks of partition p - 1 or the first 2 blocks of partition p + 1 (partitions are the aligned runs of 16 blocks; no wrap). `tile_src`: tile t names a block of partition t // 128, the partition that holds the tile. `tile_atm`: of the aligned runs of 64 tiles, no run has more than 2 tiles whose atmosphere tile has owner position in one aligned run of 16; in every draw each run reaches 2 for some owner. `atm_owner`: A permutation of the atmosphere tiles.
All inputs are finite; a program needn't handle non-finite values.
Results may differ from the reference program's by a relative error of at most 0.0042.
Values may be sent and summed in bfloat16 or wider, within the bound.
A program may use at most 64 MiB of HBM per device.

```python
import jax
import jax.numpy as jnp
from jax import lax

F = 30
BLK = 128
ACELL = 128
K = 4
NH = 2
NB = 16
TPC = 64
AT = 16
NBLK = 2048
TILES = 16384
ATILES = 2048
N_FIELD = 2


def routing(key):
    owner_key, pick_key, heat_key, slot_key = jax.random.split(jax.random.fold_in(key, 7), 4)
    atm_owner = jax.random.permutation(owner_key, ATILES).astype(jnp.int32)
    inverse = jnp.argsort(atm_owner).astype(jnp.int32)
    devices = ATILES // AT
    cores = TILES // TPC
    capacity = max(2, 4 * TPC // devices)
    groups = TPC // capacity
    heat = jax.random.randint(heat_key, (devices,), 0, 3)
    noise = jax.random.randint(pick_key, (cores, devices), 0, 1024)
    scores = (noise + 512 * heat[None, :]) * devices + jnp.arange(devices)[None, :]
    _, chosen = lax.top_k(scores, groups)
    target = jnp.repeat(chosen, capacity, axis=1)
    local_slot = jax.random.randint(slot_key, (cores, TPC), 0, AT)
    slots = (target * AT + local_slot).reshape(TILES).astype(jnp.int32)
    return (atm_owner, inverse[slots].astype(jnp.int32))


def draw_atm_owner(key, part):
    return routing(key)[0]


def draw_tile_atm(key, part):
    return routing(key)[1]


def draw_tile_src(key, part):
    devices = NBLK // NB
    per_device = TILES // devices
    device = jnp.arange(TILES) // per_device
    offset = jax.random.randint(jax.random.fold_in(key, 5), (TILES,), 0, NB)
    return (device * NB + offset).astype(jnp.int32)


def draw_neighbours(key, part):
    block_ids = jnp.arange(NBLK)[:, None]
    device = block_ids // NB
    pick = jax.random.randint(jax.random.fold_in(key, 3), (NBLK, K), 0, NB + 2 * NH)
    before = (device - 1) * NB + NB - NH + pick
    inside = device * NB + pick - NH
    after = (device + 1) * NB + pick - NH - NB
    chosen = jnp.where(pick < NH, before, jnp.where(pick < NH + NB, inside, after))
    own_block = device * NB + pick % NB
    outside = (chosen < 0) | (chosen >= NBLK)
    return jnp.where(outside, own_block, chosen).astype(jnp.int32)


def level_of(rng, dims, shards, least, largest):
    level = 1.0
    for axis_at, parts in shards:
        heights = jax.random.uniform(jax.random.fold_in(jax.random.fold_in(rng, 6), axis_at), (parts,), jnp.float32, least / len(shards), largest / len(shards))
        level = level * jnp.repeat(jnp.exp(heights), dims[axis_at] // parts).reshape((-1,) + (1,) * (len(dims) - 1 - axis_at))
    return level


def normal_values(rng, extent, deviation, bound, cuts=(), dtype=jnp.bfloat16):
    result = deviation * jax.random.normal(rng, extent, jnp.float32)
    if cuts:
        result = result * level_of(rng, extent, cuts, -0.22, 0.18)
    return jnp.clip(result, -bound, bound).astype(dtype)


def setup_inputs(seed: int = 0) -> dict:
    streams_of = jax.random.split(jax.random.key(seed), 8)
    ocean = normal_values(streams_of[0], (F, NBLK * BLK), 1.0, 6.0, ((0, 2), (1, 128)))
    grad_weight = normal_values(streams_of[1], (NBLK, K, BLK, 2 * BLK), (K * BLK) ** -0.5, 0.25, ((0, 128),))
    neighbours = draw_neighbours(jax.random.fold_in(streams_of[7], 71), 0)
    remap_weight = normal_values(streams_of[3], (TILES, 3 * BLK, ACELL), (3 * BLK * TPC * N_FIELD // AT) ** -0.5, 0.109375, ((0, 256),))
    tile_src = draw_tile_src(jax.random.fold_in(streams_of[7], 71), 0)
    tile_atm = draw_tile_atm(jax.random.fold_in(streams_of[7], 71), 0)
    atm_owner = draw_atm_owner(jax.random.fold_in(streams_of[7], 71), 0)
    return dict(ocean=ocean, grad_weight=grad_weight, neighbours=neighbours, remap_weight=remap_weight, tile_src=tile_src, tile_atm=tile_atm, atm_owner=atm_owner)


def reference(ocean, grad_weight, neighbours, remap_weight, tile_src, tile_atm, atm_owner):
    fields = ocean.shape[0]
    blocks = ocean.reshape(fields, NBLK, BLK)
    picked = blocks[:, neighbours]
    grouped_vals = picked.reshape(fields, NBLK // NB, NB, K, BLK).transpose(1, 0, 2, 3, 4)
    grouped_weights = grad_weight.reshape(NBLK // NB, NB, K, BLK, 2 * BLK)

    def gradient_group(pieces):
        group_vals, group_weights = pieces
        return jnp.einsum('fbkj,bkjo->fbo', group_vals.astype(jnp.float32), group_weights.astype(jnp.float32))

    gradient = lax.map(gradient_group, (grouped_vals, grouped_weights))
    gradient = gradient.transpose(1, 0, 2, 3).reshape(fields, NBLK, 2 * BLK).astype(jnp.bfloat16)
    source = jnp.concatenate([blocks, gradient], axis=2)
    atm_slot = atm_owner[tile_atm].astype(jnp.int32)
    groups = TILES // TPC

    def add_group(summed, pieces):
        weights, src_ids, slots = pieces
        source_rows = source[:, src_ids].astype(jnp.float32)
        contribution = jnp.einsum('ftj,tjc->tfc', source_rows, weights.astype(jnp.float32), precision=lax.Precision.HIGHEST)
        return summed.at[slots].add(contribution), None

    initial = jnp.zeros((ATILES, fields, ACELL), jnp.float32)
    summed, _ = lax.scan(add_group, initial, (remap_weight.reshape(groups, TPC, 3 * BLK, ACELL), tile_src.reshape(groups, TPC), atm_slot.reshape(groups, TPC)))
    return summed.transpose(1, 0, 2).reshape(fields, ATILES * ACELL)
```

```python
import functools

import jax
import jax.numpy as jnp
from jax import lax
from jax.experimental import pallas as pl
from jax.experimental.pallas import tpu as pltpu
from jax.sharding import PartitionSpec as P

MESH = pl.DeviceIdType.MESH
NX, NZ, NY = 4, 8, 4
PLANE = NX * NY
HALF = 15
BLK = 128
NB = 16
NH = 2
EXT = NB + 2 * NH
TILES = 64
SLOTS = 16
SRC_ROWS = 16
FCH = 3
CHUNKS = HALF // FCH
PITCH = 40
OPITCH = 24


def coords():
    d = lax.axis_index("dom")
    return lax.div(d, NZ * NY), lax.rem(lax.div(d, NY), NZ), lax.rem(d, NY)


def chip(x, z, y):
    return (x * NZ + z) * NY + y


def kernel(
    ocean_hbm,
    gw_hbm,
    nb_ref,
    rw_hbm,
    src_ref,
    rows_ref,
    meta_ref,
    out_ref,
    raw,
    wide,
    gw,
    rw,
    grads,
    cont,
    fields,
    pack,
    sent,
    sent_meta,
    got,
    got_meta,
    select,
    part,
    own,
    zgot,
    last,
    load_sem,
    w_sem,
    oc_send,
    oc_recv,
    gr_send,
    gr_recv,
    me_send,
    me_recv,
    pl_send,
    pl_recv,
    z_send,
    z_recv,
):
    c = lax.axis_index("field")
    d = lax.axis_index("dom")
    x, z, y = coords()
    other = 1 - c
    devices = NX * NZ * NY
    up, down = lax.rem(d + 1, devices), lax.rem(d + devices - 1, devices)

    def plane_chip(j):
        return chip(lax.rem(x + lax.div(j, NY), NX), z, lax.rem(y + lax.rem(j, NY), NY))

    def line_chip(dz):
        return chip(x, lax.rem(z + dz, NZ), y)

    ocean_in = pltpu.make_async_copy(
        ocean_hbm, raw.at[c, :, pl.ds(NH * BLK, NB * BLK)], load_sem.at[0]
    )
    ocean_in.start()
    gw_in = pltpu.make_async_copy(
        gw_hbm.at[pl.ds(c * (NB // 2), NB // 2)], gw, load_sem.at[1]
    )
    gw_in.start()
    rw_in = pltpu.make_async_copy(rw_hbm, rw, w_sem)
    rw_in.start()

    barrier = pltpu.get_barrier_semaphore()

    def greet(dom, core):
        pl.semaphore_signal(
            barrier, inc=1, device_id={"dom": dom, "field": core}, device_id_type=MESH
        )

    greet(d, other)
    for h in range(2):
        greet(up, h)
        greet(down, h)

    def greet_plane(j, _):
        greet(plane_chip(j), 0)
        greet(plane_chip(j), 1)
        return 0

    lax.fori_loop(1, PLANE, greet_plane, 0)

    def greet_line(dz, _):
        greet(line_chip(dz), c)
        return 0

    lax.fori_loop(1, NZ, greet_line, 0)

    target = rows_ref[...]
    row_of = lax.broadcasted_iota(jnp.int32, (PLANE * SRC_ROWS, TILES), 0)
    pack[...] = jnp.where(row_of == target, 1.0, 0.0).astype(jnp.bfloat16)
    packed_meta = jnp.dot(pack[...], meta_ref[...], preferred_element_type=jnp.float32)
    sent_meta[...] = packed_meta.astype(jnp.bfloat16)
    ocean_in.wait()

    pl.semaphore_wait(barrier, 1 + 4 + 2 * (PLANE - 1) + (NZ - 1))

    def remote(src, dst, send, recv, dom, core):
        return pltpu.make_async_remote_copy(
            src_ref=src,
            dst_ref=dst,
            send_sem=send,
            recv_sem=recv,
            device_id={"dom": dom, "field": core},
            device_id_type=MESH,
        )

    first = pl.ds(NH * BLK, NH * BLK)
    final = pl.ds(NB * BLK, NH * BLK)
    left = pl.ds(0, NH * BLK)
    right = pl.ds((NB + NH) * BLK, NH * BLK)
    middle = pl.ds(NH * BLK, NB * BLK)
    ocean_copies = [
        remote(raw.at[c, :, final], raw.at[c, :, left], oc_send.at[0], oc_recv.at[0], up, c),
        remote(raw.at[c, :, final], raw.at[c, :, left], oc_send.at[1], oc_recv.at[1], up, other),
        remote(raw.at[c, :, first], raw.at[c, :, right], oc_send.at[2], oc_recv.at[2], down, c),
        remote(raw.at[c, :, first], raw.at[c, :, right], oc_send.at[3], oc_recv.at[3], down, other),
        remote(raw.at[c, :, middle], raw.at[c, :, middle], oc_send.at[4], oc_recv.at[4], d, other),
    ]
    for copy in ocean_copies:
        copy.start()

    meta_partner = remote(
        sent_meta.at[pl.ds(15 * SRC_ROWS, SRC_ROWS)],
        got_meta.at[pl.ds(30 * SRC_ROWS, SRC_ROWS)],
        me_send,
        me_recv,
        d,
        other,
    )
    meta_partner.start()

    def send_meta(j, _):
        dom = plane_chip(j)
        for h in range(2):
            remote(
                sent_meta.at[pl.ds(pl.multiple_of((j - 1) * SRC_ROWS, SRC_ROWS), SRC_ROWS)],
                got_meta.at[
                    pl.ds(pl.multiple_of(((j - 1) * 2 + c) * SRC_ROWS, SRC_ROWS), SRC_ROWS)
                ],
                me_send,
                me_recv,
                dom,
                h,
            ).start()
        return 0

    lax.fori_loop(1, PLANE, send_meta, 0)
    got_meta[pl.ds(31 * SRC_ROWS, SRC_ROWS), :] = sent_meta[pl.ds(15 * SRC_ROWS, SRC_ROWS), :]

    for copy in ocean_copies:
        copy.wait()
    wide[...] = jnp.zeros_like(wide)
    for e in range(EXT):
        wide[e, 0:HALF, :] = raw[0, :, e * BLK : (e + 1) * BLK]
        wide[e, 16 : 16 + HALF, :] = raw[1, :, e * BLK : (e + 1) * BLK]
    gw_in.wait()

    first_block = d * NB - NH

    def gradient(i, _):
        b = c * (NB // 2) + i
        picked = jnp.concatenate(
            [wide[jnp.maximum(nb_ref[b, k] - first_block, 0)] for k in range(4)], axis=1
        )
        grads[b] = jnp.dot(picked, gw[i], preferred_element_type=jnp.float32).astype(
            jnp.bfloat16
        )
        return 0

    lax.fori_loop(0, NB // 2, gradient, 0, unroll=4)
    mine = pl.ds(c * (NB // 2), NB // 2)
    grad_copy = remote(grads.at[mine], grads.at[mine], gr_send, gr_recv, d, other)
    grad_copy.start()

    all_but_own = pl.ds(0, 31 * SRC_ROWS)
    pltpu.make_async_copy(got_meta.at[all_but_own], got_meta.at[all_but_own], me_recv).wait()
    rows_all = 32 * SRC_ROWS
    lane = lax.broadcasted_iota(jnp.int32, (rows_all, NZ * SLOTS), 1)
    row = lax.broadcasted_iota(jnp.int32, (rows_all, NZ * SLOTS), 0)
    wanted = (lax.rem(lane, SLOTS) + 1).astype(jnp.float32)
    same_z = lax.div(lax.rem(row, SRC_ROWS), 2) == lax.div(lane, SLOTS)
    chosen = jnp.where(
        same_z & (got_meta[...].astype(jnp.float32) == wanted), 1.0, 0.0
    )
    select[...] = chosen.T.astype(jnp.bfloat16)

    rw_in.wait()
    grad_copy.wait()

    own_block = d * NB

    def remap(t, _):
        s = jnp.maximum(src_ref[0, t] - own_block, 0)
        source = jnp.concatenate([wide[s + NH], grads[s]], axis=1)
        cont[pl.ds(pl.multiple_of(t * PITCH, 8), 32), :] = jnp.dot(
            source, rw[t], preferred_element_type=jnp.float32
        )
        return 0

    lax.fori_loop(0, TILES, remap, 0, unroll=8)

    def turn(g, _):
        for h in range(2):
            fields[h * HALF + g] = cont[pl.ds(h * 16 + g, TILES, stride=PITCH), :].astype(
                jnp.bfloat16
            )
        return 0

    own_rows = pl.ds(15 * SRC_ROWS, SRC_ROWS)
    for k in range(CHUNKS):
        lax.fori_loop(k * FCH, (k + 1) * FCH, turn, 0, unroll=True)
        for h in range(2):
            for g in range(k * FCH, (k + 1) * FCH):
                f = h * HALF + g
                sent[f] = jnp.dot(
                    pack[...], fields[f], preferred_element_type=jnp.float32
                ).astype(jnp.bfloat16)
        chunk = pl.ds(k * FCH, FCH)

        remote(
            sent.at[pl.ds(other * HALF + k * FCH, FCH), own_rows],
            got.at[chunk, pl.ds(30 * SRC_ROWS, SRC_ROWS)],
            pl_send.at[k],
            pl_recv.at[k],
            d,
            other,
        ).start()

        def send(j, _, k=k, chunk=chunk):
            dom = plane_chip(j)
            for h in range(2):
                remote(
                    sent.at[
                        pl.ds(h * HALF + k * FCH, FCH),
                        pl.ds(pl.multiple_of((j - 1) * SRC_ROWS, SRC_ROWS), SRC_ROWS),
                    ],
                    got.at[
                        chunk,
                        pl.ds(pl.multiple_of(((j - 1) * 2 + c) * SRC_ROWS, SRC_ROWS), SRC_ROWS),
                    ],
                    pl_send.at[k],
                    pl_recv.at[k],
                    dom,
                    h,
                ).start()
            return 0

        lax.fori_loop(1, PLANE, send, 0)
        got[chunk, pl.ds(31 * SRC_ROWS, SRC_ROWS), :] = sent[
            pl.ds(c * HALF + k * FCH, FCH), own_rows, :
        ]

    for k in range(CHUNKS):
        chunk = pl.ds(k * FCH, FCH)
        arrived = got.at[chunk, all_but_own]
        pltpu.make_async_copy(arrived, arrived, pl_recv.at[k]).wait()
        for g in range(k * FCH, (k + 1) * FCH):
            total = jnp.dot(select[...], got[g], preferred_element_type=jnp.float32)
            own[g] = total[0:SLOTS]
            part[g] = total.astype(jnp.bfloat16)

        def send_z(dz, _, k=k, chunk=chunk):
            remote(
                part.at[chunk, pl.ds(pl.multiple_of(dz * SLOTS, SLOTS), SLOTS)],
                zgot.at[chunk, pl.ds(pl.multiple_of((dz - 1) * SLOTS, SLOTS), SLOTS)],
                z_send.at[k],
                z_recv.at[k],
                line_chip(dz),
                c,
            ).start()
            return 0

        lax.fori_loop(1, NZ, send_z, 0)

    for k in range(CHUNKS):
        chunk = pl.ds(k * FCH, FCH)
        pltpu.make_async_copy(zgot.at[chunk], zgot.at[chunk], z_recv.at[k]).wait()
        for g in range(k * FCH, (k + 1) * FCH):
            total = own[g]
            for s in range(NZ - 1):
                total = total + zgot[g, s * SLOTS : (s + 1) * SLOTS, :].astype(jnp.float32)
            last[g * OPITCH : g * OPITCH + SLOTS, :] = total
    last[HALF * OPITCH :, :] = jnp.zeros((OPITCH, BLK), jnp.float32)
    for s in range(SLOTS):
        line = last[pl.ds(s, 16, stride=OPITCH), :]
        out_ref[:, s * BLK : (s + 1) * BLK] = line[0:HALF]

    pltpu.make_async_copy(got_meta.at[all_but_own], got_meta.at[all_but_own], me_send).wait()
    for k in range(CHUNKS):
        chunk = pl.ds(k * FCH, FCH)
        arrived = got.at[chunk, all_but_own]
        pltpu.make_async_copy(arrived, arrived, pl_send.at[k]).wait()
        pltpu.make_async_copy(zgot.at[chunk], zgot.at[chunk], z_send.at[k]).wait()


def local(ocean, grad_weight, neighbours, remap_weight, tile_src, tile_atm, atm_owner):
    x, z, y = coords()
    slot = jnp.sum(
        jnp.where(
            tile_atm[:, None] == jnp.arange(atm_owner.shape[0], dtype=jnp.int32)[None, :],
            atm_owner[None, :],
            0,
        ),
        axis=1,
    )
    owner, local_slot = slot // SLOTS, slot % SLOTS
    order = jnp.arange(TILES, dtype=jnp.int32)
    rank = jnp.sum(
        ((owner[:, None] == owner[None, :]) & (order[:, None] < order[None, :])).astype(jnp.int32),
        axis=0,
    )
    ox, oz, oy = owner // (NZ * NY), (owner // NY) % NZ, owner % NY
    j = ((ox - x) % NX) * NY + (oy - y) % NY
    rows = ((j + 15) % 16) * SRC_ROWS + ((oz - z) % NZ) * 2 + rank
    meta = jnp.broadcast_to((local_slot + 1).astype(jnp.bfloat16)[:, None], (TILES, BLK))
    bf16, f32 = jnp.bfloat16, jnp.float32
    vmem, smem, hbm = (
        pl.BlockSpec(memory_space=pltpu.VMEM),
        pl.BlockSpec(memory_space=pltpu.SMEM),
        pl.BlockSpec(memory_space=pl.ANY),
    )
    dma = pltpu.SemaphoreType.DMA
    return pl.pallas_call(
        kernel,
        out_shape=jax.ShapeDtypeStruct((HALF, NB * BLK), f32),
        in_specs=[hbm, hbm, smem, hbm, smem, vmem, vmem],
        out_specs=vmem,
        scratch_shapes=[
            pltpu.VMEM((2, HALF, EXT * BLK), bf16),
            pltpu.VMEM((EXT, 32, BLK), bf16),
            pltpu.VMEM((NB // 2, 4 * BLK, 2 * BLK), bf16),
            pltpu.VMEM((TILES, 3 * BLK, BLK), bf16),
            pltpu.VMEM((NB, 32, 2 * BLK), bf16),
            pltpu.VMEM((TILES * PITCH, BLK), f32),
            pltpu.VMEM((2 * HALF, TILES, BLK), bf16),
            pltpu.VMEM((PLANE * SRC_ROWS, TILES), bf16),
            pltpu.VMEM((2 * HALF, PLANE * SRC_ROWS, BLK), bf16),
            pltpu.VMEM((PLANE * SRC_ROWS, BLK), bf16),
            pltpu.VMEM((HALF, 32 * SRC_ROWS, BLK), bf16),
            pltpu.VMEM((32 * SRC_ROWS, BLK), bf16),
            pltpu.VMEM((NZ * SLOTS, 32 * SRC_ROWS), bf16),
            pltpu.VMEM((HALF, NZ * SLOTS, BLK), bf16),
            pltpu.VMEM((HALF, SLOTS, BLK), f32),
            pltpu.VMEM((HALF, (NZ - 1) * SLOTS, BLK), bf16),
            pltpu.VMEM((16 * OPITCH, BLK), f32),
            dma((2,)),
            dma,
            dma((5,)),
            dma((5,)),
            dma,
            dma,
            dma,
            dma,
            dma((CHUNKS,)),
            dma((CHUNKS,)),
            dma((CHUNKS,)),
            dma((CHUNKS,)),
        ],
        compiler_params=pltpu.CompilerParams(
            collective_id=0, has_side_effects=True, vmem_limit_bytes=40 * 1024 * 1024
        ),
    )(
        ocean,
        grad_weight.reshape(NB, 4 * BLK, 2 * BLK),
        neighbours,
        remap_weight,
        tile_src[None, :],
        rows[None, :],
        meta,
    )


def solution(mesh):
    in_specs = (
        P("field", "dom"),
        P("dom", None, None, None),
        P("dom", None),
        P(("dom", "field"), None, None),
        P(("dom", "field")),
        P(("dom", "field")),
        P(),
    )
    out_specs = P("field", "dom")
    return jax.shard_map(local, mesh=mesh, in_specs=in_specs, out_specs=out_specs, check_vma=False)
```

```python
import functools

import jax
import jax.numpy as jnp
from jax import lax
from jax.experimental import pallas as pl
from jax.experimental.pallas import tpu as pltpu
from jax.sharding import PartitionSpec as P

MESH = pl.DeviceIdType.MESH
NX, NZ, NY = 4, 8, 4
PLANE = NX * NY
HALF = 15
BLK = 128
NB = 16
NH = 2
EXT = NB + 2 * NH
TILES = 64
SLOTS = 16
SRC_ROWS = 16
FCH = 3
CHUNKS = HALF // FCH
PITCH = 40
OPITCH = 24


def coords():
    d = lax.axis_index("dom")
    return lax.div(d, NZ * NY), lax.rem(lax.div(d, NY), NZ), lax.rem(d, NY)


def chip(x, z, y):
    return (x * NZ + z) * NY + y


def kernel(
    ocean_hbm,
    gw_hbm,
    nb_hbm,
    rw_hbm,
    src_hbm,
    atm_hbm,
    owner_hbm,
    out_ref,
    nb_ref,
    src_ref,
    atm,
    owners,
    raw,
    wide,
    gw,
    rw,
    grads,
    cont,
    fields,
    pack,
    sent,
    sent_meta,
    got,
    got_meta,
    select,
    part,
    own,
    zgot,
    last,
    load_sem,
    w_sem,
    oc_send,
    oc_recv,
    near_sem,
    me_send,
    me_recv,
    pl_send,
    pl_recv,
    z_send,
    z_recv,
):
    c = lax.axis_index("field")
    d = lax.axis_index("dom")
    x, z, y = coords()
    other = 1 - c
    devices = NX * NZ * NY
    up, down = lax.rem(d + 1, devices), lax.rem(d + devices - 1, devices)

    def plane_chip(j):
        return chip(lax.rem(x + lax.div(j, NY), NX), z, lax.rem(y + lax.rem(j, NY), NY))

    def line_chip(dz):
        return chip(x, lax.rem(z + dz, NZ), y)

    ocean_in = pltpu.make_async_copy(
        ocean_hbm, raw.at[c, :, pl.ds(NH * BLK, NB * BLK)], load_sem.at[0]
    )
    ocean_in.start()
    small = [
        pltpu.make_async_copy(src, dst, load_sem.at[n])
        for n, (src, dst) in enumerate(
            ((atm_hbm, atm), (owner_hbm, owners), (nb_hbm, nb_ref), (src_hbm, src_ref)), 1
        )
    ]
    for copy in small:
        copy.start()
    gw_in = pltpu.make_async_copy(gw_hbm, gw, load_sem.at[5])
    gw_in.start()
    rw_in = pltpu.make_async_copy(rw_hbm, rw, w_sem)
    rw_in.start()

    barrier = pltpu.get_barrier_semaphore()

    def greet(dom, core, sem=barrier):
        pl.semaphore_signal(
            sem, inc=1, device_id={"dom": dom, "field": core}, device_id_type=MESH
        )

    y_ring = [chip(x, z, lax.rem(y + n, NY)) for n in range(1, NY)]
    z_near = [chip(x, lax.rem(z + n, NZ), y) for n in (1, NZ - 1, 2, NZ - 2)]
    for h in range(2):
        greet(up, h)
        greet(down, h)
    for dom in z_near + y_ring:
        greet(dom, c)
    for n in range(1, NX):
        for h in range(2):
            greet(chip(lax.rem(x + n, NX), z, y), h)
    greet(d, other)

    small[0].wait()
    small[1].wait()
    bf16, f32 = jnp.bfloat16, jnp.float32

    def dot(a, b):
        return jnp.dot(a, b, preferred_element_type=f32)

    def iota(shape, dim):
        return lax.broadcasted_iota(jnp.int32, shape, dim)

    def one_hot(mask):
        return jnp.where(mask, 1.0, 0.0).astype(bf16)

    ids = atm[...]
    table = owners[...]
    halves = jnp.concatenate([table >> 4, table & 15], axis=0).astype(f32).astype(bf16)
    found = dot(halves, one_hot(iota((BLK, TILES), 0) == (ids & (BLK - 1))))
    here = iota((16, TILES), 0) == (ids >> 7)
    owner_row = jnp.sum(jnp.where(here, found[0:16], 0.0), axis=0, keepdims=True)
    slot_row = jnp.sum(jnp.where(here, found[16:32], 0.0), axis=0, keepdims=True)
    square = (TILES, TILES)
    diagonal = jnp.where(iota(square, 0) == iota(square, 1), owner_row, 0.0).astype(bf16)
    owner_col = dot(diagonal, jnp.ones(square, bf16))
    earlier = (owner_col == owner_row) & (iota(square, 0) < iota(square, 1))
    rank = jnp.sum(jnp.where(earlier, 1, 0), axis=0, keepdims=True)
    owner = owner_row.astype(jnp.int32)
    dx = ((owner >> 5) - x) & (NX - 1)
    dz = ((owner >> 2) - z) & (NZ - 1)
    dy = (owner - y) & (NY - 1)
    target = ((dx * NY + dy + PLANE - 1) & (PLANE - 1)) * SRC_ROWS + dz * 2 + rank
    chosen = iota((PLANE * SRC_ROWS, TILES), 0) == target
    pack[...] = one_hot(chosen)
    slots_at = jnp.where(chosen, slot_row + 1.0, 0.0).astype(bf16)
    sent_meta[...] = dot(slots_at, jnp.ones((TILES, BLK), bf16)).astype(bf16)
    ocean_in.wait()

    pl.semaphore_wait(barrier, 4 + 4 + 3 + 6 + 1)

    def remote(src, dst, send, recv, dom, core):
        return pltpu.make_async_remote_copy(
            src_ref=src,
            dst_ref=dst,
            send_sem=send,
            recv_sem=recv,
            device_id={"dom": dom, "field": core},
            device_id_type=MESH,
        )

    first = pl.ds(NH * BLK, NH * BLK)
    final = pl.ds(NB * BLK, NH * BLK)
    left = pl.ds(0, NH * BLK)
    right = pl.ds((NB + NH) * BLK, NH * BLK)
    middle = pl.ds(NH * BLK, NB * BLK)
    ocean_copies = [
        remote(raw.at[c, :, final], raw.at[c, :, left], oc_send.at[0], oc_recv.at[0], up, c),
        remote(raw.at[c, :, final], raw.at[c, :, left], oc_send.at[1], oc_recv.at[1], up, other),
        remote(raw.at[c, :, first], raw.at[c, :, right], oc_send.at[2], oc_recv.at[2], down, c),
        remote(raw.at[c, :, first], raw.at[c, :, right], oc_send.at[3], oc_recv.at[3], down, other),
        remote(raw.at[c, :, middle], raw.at[c, :, middle], oc_send.at[4], oc_recv.at[4], d, other),
    ]
    for copy in ocean_copies:
        copy.start()

    for dom in y_ring + z_near[2:]:
        greet(dom, c, near_sem)
    pl.semaphore_wait(near_sem, 5)

    meta_partner = remote(
        sent_meta.at[pl.ds(15 * SRC_ROWS, SRC_ROWS)],
        got_meta.at[pl.ds(30 * SRC_ROWS, SRC_ROWS)],
        me_send,
        me_recv,
        d,
        other,
    )
    meta_partner.start()

    def send_meta(j, _):
        dom = plane_chip(j)
        for h in range(2):
            remote(
                sent_meta.at[pl.ds(pl.multiple_of((j - 1) * SRC_ROWS, SRC_ROWS), SRC_ROWS)],
                got_meta.at[
                    pl.ds(pl.multiple_of(((j - 1) * 2 + c) * SRC_ROWS, SRC_ROWS), SRC_ROWS)
                ],
                me_send,
                me_recv,
                dom,
                h,
            ).start()
        return 0

    lax.fori_loop(1, PLANE, send_meta, 0)
    got_meta[pl.ds(31 * SRC_ROWS, SRC_ROWS), :] = sent_meta[pl.ds(15 * SRC_ROWS, SRC_ROWS), :]

    for copy in ocean_copies:
        copy.wait()
    wide[...] = jnp.zeros_like(wide)
    for e in range(EXT):
        wide[e, 0:HALF, :] = raw[0, :, e * BLK : (e + 1) * BLK]
        wide[e, 16 : 16 + HALF, :] = raw[1, :, e * BLK : (e + 1) * BLK]
    gw_in.wait()

    first_block = d * NB - NH

    small[2].wait()
    small[3].wait()

    def gradient(b, _):
        picked = jnp.concatenate(
            [wide[jnp.maximum(nb_ref[k, b] - first_block, 0)] for k in range(4)], axis=1
        )
        grads[b] = jnp.dot(picked, gw[b], preferred_element_type=jnp.float32).astype(
            jnp.bfloat16
        )
        return 0

    lax.fori_loop(0, NB, gradient, 0, unroll=4)
    all_but_own = pl.ds(0, 31 * SRC_ROWS)
    pltpu.make_async_copy(got_meta.at[all_but_own], got_meta.at[all_but_own], me_recv).wait()
    rows_all = 32 * SRC_ROWS
    lane, row = iota((rows_all, NZ * SLOTS), 1), iota((rows_all, NZ * SLOTS), 0)
    wanted = ((lane & (SLOTS - 1)) + 1).astype(f32)
    same_z = ((row & (SRC_ROWS - 1)) >> 1) == (lane >> 4)
    chosen = jnp.where(same_z & (got_meta[...].astype(f32) == wanted), 1.0, 0.0)
    select[...] = chosen.T.astype(bf16)

    rw_in.wait()

    own_block = d * NB

    def remap(t, _):
        s = jnp.maximum(src_ref[0, t] - own_block, 0)
        source = jnp.concatenate([wide[s + NH], grads[s]], axis=1)
        cont[pl.ds(pl.multiple_of(t * PITCH, 8), 32), :] = jnp.dot(
            source, rw[t], preferred_element_type=jnp.float32
        )
        return 0

    lax.fori_loop(0, TILES, remap, 0, unroll=8)

    def turn(g, _):
        for h in range(2):
            fields[h * HALF + g] = cont[pl.ds(h * 16 + g, TILES, stride=PITCH), :].astype(
                jnp.bfloat16
            )
        return 0

    own_rows = pl.ds(15 * SRC_ROWS, SRC_ROWS)
    for k in range(CHUNKS):
        lax.fori_loop(k * FCH, (k + 1) * FCH, turn, 0, unroll=True)
        for h in range(2):
            for g in range(k * FCH, (k + 1) * FCH):
                f = h * HALF + g
                sent[f] = jnp.dot(
                    pack[...], fields[f], preferred_element_type=jnp.float32
                ).astype(jnp.bfloat16)
        chunk = pl.ds(k * FCH, FCH)

        remote(
            sent.at[pl.ds(other * HALF + k * FCH, FCH), own_rows],
            got.at[chunk, pl.ds(30 * SRC_ROWS, SRC_ROWS)],
            pl_send.at[k],
            pl_recv.at[k],
            d,
            other,
        ).start()

        def send(j, _, k=k, chunk=chunk):
            dom = plane_chip(j)
            for h in range(2):
                remote(
                    sent.at[
                        pl.ds(h * HALF + k * FCH, FCH),
                        pl.ds(pl.multiple_of((j - 1) * SRC_ROWS, SRC_ROWS), SRC_ROWS),
                    ],
                    got.at[
                        chunk,
                        pl.ds(pl.multiple_of(((j - 1) * 2 + c) * SRC_ROWS, SRC_ROWS), SRC_ROWS),
                    ],
                    pl_send.at[k],
                    pl_recv.at[k],
                    dom,
                    h,
                ).start()
            return 0

        lax.fori_loop(1, PLANE, send, 0)
        got[chunk, pl.ds(31 * SRC_ROWS, SRC_ROWS), :] = sent[
            pl.ds(c * HALF + k * FCH, FCH), own_rows, :
        ]

    for k in range(CHUNKS):
        chunk = pl.ds(k * FCH, FCH)
        arrived = got.at[chunk, all_but_own]
        pltpu.make_async_copy(arrived, arrived, pl_recv.at[k]).wait()
        for g in range(k * FCH, (k + 1) * FCH):
            total = jnp.dot(select[...], got[g], preferred_element_type=jnp.float32)
            own[g] = total[0:SLOTS]
            part[g] = total.astype(jnp.bfloat16)

        def send_z(dz, _, k=k, chunk=chunk):
            remote(
                part.at[chunk, pl.ds(pl.multiple_of(dz * SLOTS, SLOTS), SLOTS)],
                zgot.at[chunk, pl.ds(pl.multiple_of((dz - 1) * SLOTS, SLOTS), SLOTS)],
                z_send.at[k],
                z_recv.at[k],
                line_chip(dz),
                c,
            ).start()
            return 0

        lax.fori_loop(1, NZ, send_z, 0)

    for k in range(CHUNKS):
        chunk = pl.ds(k * FCH, FCH)
        pltpu.make_async_copy(zgot.at[chunk], zgot.at[chunk], z_recv.at[k]).wait()
        for g in range(k * FCH, (k + 1) * FCH):
            total = own[g]
            for s in range(NZ - 1):
                total = total + zgot[g, s * SLOTS : (s + 1) * SLOTS, :].astype(jnp.float32)
            last[g * OPITCH : g * OPITCH + SLOTS, :] = total
    last[HALF * OPITCH :, :] = jnp.zeros((OPITCH, BLK), jnp.float32)
    for s in range(SLOTS):
        line = last[pl.ds(s, 16, stride=OPITCH), :]
        out_ref[:, s * BLK : (s + 1) * BLK] = line[0:HALF]

    pltpu.make_async_copy(got_meta.at[all_but_own], got_meta.at[all_but_own], me_send).wait()
    for k in range(CHUNKS):
        chunk = pl.ds(k * FCH, FCH)
        arrived = got.at[chunk, all_but_own]
        pltpu.make_async_copy(arrived, arrived, pl_send.at[k]).wait()
        pltpu.make_async_copy(zgot.at[chunk], zgot.at[chunk], z_send.at[k]).wait()


def local(ocean, grad_weight, neighbours, remap_weight, tile_src, tile_atm, atm_owner):
    bf16, f32, i32 = jnp.bfloat16, jnp.float32, jnp.int32
    vmem = pl.BlockSpec(memory_space=pltpu.VMEM)
    hbm = pl.BlockSpec(memory_space=pltpu.HBM)
    dma = pltpu.SemaphoreType.DMA
    return pl.pallas_call(
        kernel,
        out_shape=jax.ShapeDtypeStruct((HALF, NB * BLK), f32),
        in_specs=[hbm] * 7,
        out_specs=vmem,
        scratch_shapes=[
            pltpu.SMEM((4, NB), i32),
            pltpu.SMEM((1, TILES), i32),
            pltpu.VMEM((1, TILES), i32),
            pltpu.VMEM((NB, BLK), i32),
            pltpu.VMEM((2, HALF, EXT * BLK), bf16),
            pltpu.VMEM((EXT, 32, BLK), bf16),
            pltpu.VMEM((NB, 4 * BLK, 2 * BLK), bf16),
            pltpu.VMEM((TILES, 3 * BLK, BLK), bf16),
            pltpu.VMEM((NB, 32, 2 * BLK), bf16),
            pltpu.VMEM((TILES * PITCH, BLK), f32),
            pltpu.VMEM((2 * HALF, TILES, BLK), bf16),
            pltpu.VMEM((PLANE * SRC_ROWS, TILES), bf16),
            pltpu.VMEM((2 * HALF, PLANE * SRC_ROWS, BLK), bf16),
            pltpu.VMEM((PLANE * SRC_ROWS, BLK), bf16),
            pltpu.VMEM((HALF, 32 * SRC_ROWS, BLK), bf16),
            pltpu.VMEM((32 * SRC_ROWS, BLK), bf16),
            pltpu.VMEM((NZ * SLOTS, 32 * SRC_ROWS), bf16),
            pltpu.VMEM((HALF, NZ * SLOTS, BLK), bf16),
            pltpu.VMEM((HALF, SLOTS, BLK), f32),
            pltpu.VMEM((HALF, (NZ - 1) * SLOTS, BLK), bf16),
            pltpu.VMEM((16 * OPITCH, BLK), f32),
            dma((6,)),
            dma,
            dma((5,)),
            dma((5,)),
            pltpu.SemaphoreType.REGULAR,
            dma,
            dma,
            dma((CHUNKS,)),
            dma((CHUNKS,)),
            dma((CHUNKS,)),
            dma((CHUNKS,)),
        ],
        compiler_params=pltpu.CompilerParams(
            collective_id=0, has_side_effects=True, vmem_limit_bytes=67_043_328
        ),
    )(
        ocean,
        grad_weight.reshape(NB, 4 * BLK, 2 * BLK),
        neighbours.T,
        remap_weight,
        tile_src[None, :],
        tile_atm[None, :],
        atm_owner.reshape(NB, BLK),
    )


def solution(mesh):
    in_specs = (
        P("field", "dom"),
        P("dom", None, None, None),
        P("dom", None),
        P(("dom", "field"), None, None),
        P(("dom", "field")),
        P(("dom", "field")),
        P(),
    )
    out_specs = P("field", "dom")
    return jax.shard_map(local, mesh=mesh, in_specs=in_specs, out_specs=out_specs, check_vma=False)
```

```python
import functools

import jax
import jax.numpy as jnp
from jax import lax
from jax.experimental import pallas as pl
from jax.experimental.pallas import tpu as pltpu
from jax.sharding import PartitionSpec as P

MESH = pl.DeviceIdType.MESH
NX, NZ, NY = 4, 8, 4
PLANE = NX * NY
HALF = 15
BLK = 128
NB = 16
NH = 2
EXT = NB + 2 * NH
TILES = 64
SLOTS = 16
SRC_ROWS = 16
SPLIT = ((0, 3), (3, 3), (6, 3), (9, 2), (11, 1))
CHUNKS = len(SPLIT)
ZF, ZN = 12, 3
PITCH = 40
OPITCH = 24


def coords():
    d = lax.axis_index("dom")
    return lax.div(d, NZ * NY), lax.rem(lax.div(d, NY), NZ), lax.rem(d, NY)


def chip(x, z, y):
    return (x * NZ + z) * NY + y


def kernel(
    ocean_hbm,
    gw_hbm,
    nb_hbm,
    rw_hbm,
    src_hbm,
    atm_hbm,
    owner_hbm,
    out_ref,
    nb_ref,
    src_ref,
    atm,
    owners,
    raw,
    wide,
    gw,
    rw,
    grads,
    cont,
    fields,
    pack,
    sent,
    sent_meta,
    got,
    got_meta,
    select,
    part,
    own,
    zgot,
    last,
    zpack,
    zsent,
    zsent_meta,
    zraw,
    zraw_meta,
    zselect,
    zpart,
    zown,
    zlast,
    load_sem,
    w_sem,
    oc_send,
    oc_recv,
    near_sem,
    me_send,
    me_recv,
    pl_send,
    pl_recv,
    z_send,
    z_recv,
    zm_send,
    zm_recv,
    zr_send,
    zr_recv,
    zp_send,
    zp_recv,
):
    c = lax.axis_index("field")
    d = lax.axis_index("dom")
    x, z, y = coords()
    other = 1 - c
    devices = NX * NZ * NY
    up, down = lax.rem(d + 1, devices), lax.rem(d + devices - 1, devices)

    def plane_chip(j):
        return chip(lax.rem(x + lax.div(j, NY), NX), z, lax.rem(y + lax.rem(j, NY), NY))

    def line_chip(dz):
        return chip(x, lax.rem(z + dz, NZ), y)

    ocean_in = pltpu.make_async_copy(
        ocean_hbm, raw.at[c, :, pl.ds(NH * BLK, NB * BLK)], load_sem.at[0]
    )
    ocean_in.start()
    small = [
        pltpu.make_async_copy(src, dst, load_sem.at[n])
        for n, (src, dst) in enumerate(
            ((atm_hbm, atm), (owner_hbm, owners), (nb_hbm, nb_ref), (src_hbm, src_ref)), 1
        )
    ]
    for copy in small:
        copy.start()
    gw_in = pltpu.make_async_copy(gw_hbm, gw, load_sem.at[5])
    gw_in.start()
    rw_in = pltpu.make_async_copy(rw_hbm, rw, w_sem)
    rw_in.start()

    barrier = pltpu.get_barrier_semaphore()

    def greet(dom, core, sem=barrier):
        pl.semaphore_signal(
            sem, inc=1, device_id={"dom": dom, "field": core}, device_id_type=MESH
        )

    y_ring = [chip(x, z, lax.rem(y + n, NY)) for n in range(1, NY)]
    z_near = [chip(x, lax.rem(z + n, NZ), y) for n in (1, NZ - 1, 2, NZ - 2)]
    for h in range(2):
        greet(up, h)
        greet(down, h)
    for dom in z_near:
        greet(dom, 0)
        greet(dom, 1)
    for dom in y_ring:
        greet(dom, c)
    for n in range(1, NX):
        for h in range(2):
            greet(chip(lax.rem(x + n, NX), z, y), h)
    greet(d, other)

    small[0].wait()
    small[1].wait()
    bf16, f32 = jnp.bfloat16, jnp.float32

    def dot(a, b):
        return jnp.dot(a, b, preferred_element_type=f32)

    def iota(shape, dim):
        return lax.broadcasted_iota(jnp.int32, shape, dim)

    def one_hot(mask):
        return jnp.where(mask, 1.0, 0.0).astype(bf16)

    ids = atm[...]
    table = owners[...]
    halves = jnp.concatenate([table >> 4, table & 15], axis=0).astype(f32).astype(bf16)
    found = dot(halves, one_hot(iota((BLK, TILES), 0) == (ids & (BLK - 1))))
    here = iota((16, TILES), 0) == (ids >> 7)
    owner_row = jnp.sum(jnp.where(here, found[0:16], 0.0), axis=0, keepdims=True)
    slot_row = jnp.sum(jnp.where(here, found[16:32], 0.0), axis=0, keepdims=True)
    square = (TILES, TILES)
    diagonal = jnp.where(iota(square, 0) == iota(square, 1), owner_row, 0.0).astype(bf16)
    owner_col = dot(diagonal, jnp.ones(square, bf16))
    earlier = (owner_col == owner_row) & (iota(square, 0) < iota(square, 1))
    rank = jnp.sum(jnp.where(earlier, 1, 0), axis=0, keepdims=True)
    owner = owner_row.astype(jnp.int32)
    dx = ((owner >> 5) - x) & (NX - 1)
    dz = ((owner >> 2) - z) & (NZ - 1)
    dy = (owner - y) & (NY - 1)
    jj = (dx * NY + dy + PLANE - 1) & (PLANE - 1)
    z_rel = (dz + NZ - 1) & (NZ - 1)
    within = (dz * 2 + rank, jj * 2 + rank)
    plans = (
        (jj, within[0], SRC_ROWS, pack, sent_meta),
        (z_rel, within[1], 2 * PLANE, zpack, zsent_meta),
    )
    for group, inner, width, matrix, metas in plans:
        matrix[...] = one_hot(iota((PLANE * SRC_ROWS, TILES), 0) == group * width + inner)
        marked = jnp.where(iota((PLANE, TILES), 0) == group, slot_row + 1.0, 0.0).astype(bf16)
        spread = jnp.where(iota(square, 0) == iota(square, 1), inner.astype(f32), 0.0)
        inner_col = dot(spread.astype(bf16), jnp.ones((TILES, BLK), bf16))
        lanes = (iota((TILES, BLK), 1) & (width - 1)).astype(f32)
        table = dot(marked, one_hot(inner_col == lanes))
        for n in range(metas.shape[0]):
            metas[n] = table[n : n + 1]
    ocean_in.wait()

    pl.semaphore_wait(barrier, 4 + 8 + 3 + 6 + 1)

    def remote(src, dst, send, recv, dom, core):
        return pltpu.make_async_remote_copy(
            src_ref=src,
            dst_ref=dst,
            send_sem=send,
            recv_sem=recv,
            device_id={"dom": dom, "field": core},
            device_id_type=MESH,
        )

    first = pl.ds(NH * BLK, NH * BLK)
    final = pl.ds(NB * BLK, NH * BLK)
    left = pl.ds(0, NH * BLK)
    right = pl.ds((NB + NH) * BLK, NH * BLK)
    middle = pl.ds(NH * BLK, NB * BLK)
    ocean_copies = [
        remote(raw.at[c, :, final], raw.at[c, :, left], oc_send.at[0], oc_recv.at[0], up, c),
        remote(raw.at[c, :, final], raw.at[c, :, left], oc_send.at[1], oc_recv.at[1], up, other),
        remote(raw.at[c, :, first], raw.at[c, :, right], oc_send.at[2], oc_recv.at[2], down, c),
        remote(raw.at[c, :, first], raw.at[c, :, right], oc_send.at[3], oc_recv.at[3], down, other),
        remote(raw.at[c, :, middle], raw.at[c, :, middle], oc_send.at[4], oc_recv.at[4], d, other),
    ]
    for copy in ocean_copies:
        copy.start()

    for dom in y_ring + z_near[2:]:
        greet(dom, c, near_sem)
    for copy in ocean_copies:
        copy.wait()
    wide[...] = jnp.zeros_like(wide)
    for e in range(EXT):
        wide[e, 0:HALF, :] = raw[0, :, e * BLK : (e + 1) * BLK]
        wide[e, 16 : 16 + HALF, :] = raw[1, :, e * BLK : (e + 1) * BLK]
    gw_in.wait()

    first_block = d * NB - NH

    small[2].wait()
    small[3].wait()

    def gradient(b, _):
        picked = jnp.concatenate(
            [wide[jnp.maximum(nb_ref[k, b] - first_block, 0)] for k in range(4)], axis=1
        )
        grads[b] = jnp.dot(picked, gw[b], preferred_element_type=jnp.float32).astype(
            jnp.bfloat16
        )
        return 0

    lax.fori_loop(0, NB, gradient, 0, unroll=4)
    rw_in.wait()

    own_block = d * NB

    def remap(t, _):
        s = jnp.maximum(src_ref[0, t] - own_block, 0)
        source = jnp.concatenate([wide[s + NH], grads[s]], axis=1)
        cont[pl.ds(pl.multiple_of(t * PITCH, 8), 32), :] = jnp.dot(
            source, rw[t], preferred_element_type=jnp.float32
        )
        return 0

    lax.fori_loop(0, TILES, remap, 0, unroll=8)

    def turn(g, _):
        for h in range(2):
            fields[h * HALF + g] = cont[pl.ds(h * 16 + g, TILES, stride=PITCH), :].astype(
                jnp.bfloat16
            )
        return 0

    pl.semaphore_wait(near_sem, 5)

    remote(sent_meta.at[15], got_meta.at[30], me_send, me_recv, d, other).start()
    remote(zsent_meta.at[7], zraw_meta.at[14], zm_send, zm_recv, d, other).start()

    def send_meta(j, _):
        for h in range(2):
            remote(
                sent_meta.at[j - 1],
                got_meta.at[(j - 1) * 2 + c],
                me_send,
                me_recv,
                plane_chip(j),
                h,
            ).start()
        return 0

    def send_zmeta(dz, _):
        for h in range(2):
            remote(
                zsent_meta.at[dz - 1],
                zraw_meta.at[(dz - 1) * 2 + c],
                zm_send,
                zm_recv,
                line_chip(dz),
                h,
            ).start()
        return 0

    lax.fori_loop(1, PLANE, send_meta, 0)
    lax.fori_loop(1, NZ, send_zmeta, 0)
    got_meta[31] = sent_meta[15]
    zraw_meta[15] = zsent_meta[7]

    def z_rows(start):
        return pl.ds(pl.multiple_of(start * 32, 32), 32)

    own_rows = pl.ds(15 * SRC_ROWS, SRC_ROWS)
    all_but_own = pl.ds(0, 31 * SRC_ROWS)
    z_but_own = pl.ds(0, 15 * 32)
    zchunk = pl.ds(ZF, ZN)

    def send_plane(k):
        f0, fn = SPLIT[k]
        for g in range(f0, f0 + fn):
            turn(g, 0)
        for h in range(2):
            for g in range(f0, f0 + fn):
                f = h * HALF + g
                sent[f] = dot(pack[...], fields[f]).astype(bf16)
        chunk = pl.ds(f0, fn)
        remote(
            sent.at[pl.ds(other * HALF + f0, fn), own_rows],
            got.at[chunk, pl.ds(30 * SRC_ROWS, SRC_ROWS)],
            pl_send.at[k],
            pl_recv.at[k],
            d,
            other,
        ).start()

        def send(j, _):
            dom = plane_chip(j)
            for h in range(2):
                remote(
                    sent.at[
                        pl.ds(h * HALF + f0, fn),
                        pl.ds(pl.multiple_of((j - 1) * SRC_ROWS, SRC_ROWS), SRC_ROWS),
                    ],
                    got.at[
                        chunk,
                        pl.ds(pl.multiple_of(((j - 1) * 2 + c) * SRC_ROWS, SRC_ROWS), SRC_ROWS),
                    ],
                    pl_send.at[k],
                    pl_recv.at[k],
                    dom,
                    h,
                ).start()
            return 0

        lax.fori_loop(1, PLANE, send, 0)
        got[chunk, pl.ds(31 * SRC_ROWS, SRC_ROWS), :] = sent[
            pl.ds(c * HALF + f0, fn), own_rows, :
        ]

    send_plane(0)
    for g in range(ZF, ZF + ZN):
        turn(g, 0)
    for h in range(2):
        for g in range(ZN):
            zsent[h * ZN + g] = dot(zpack[...], fields[h * HALF + ZF + g]).astype(bf16)
    remote(
        zsent.at[pl.ds(other * ZN, ZN), z_rows(7)],
        zraw.at[:, z_rows(14)],
        zr_send,
        zr_recv,
        d,
        other,
    ).start()

    def send_raw(dz, _):
        for h in range(2):
            remote(
                zsent.at[pl.ds(h * ZN, ZN), z_rows(dz - 1)],
                zraw.at[:, z_rows((dz - 1) * 2 + c)],
                zr_send,
                zr_recv,
                line_chip(dz),
                h,
            ).start()
        return 0

    lax.fori_loop(1, NZ, send_raw, 0)
    zraw[:, z_rows(15), :] = zsent[pl.ds(c * ZN, ZN), z_rows(7), :]
    for k in range(1, CHUNKS):
        send_plane(k)

    most, z_most = got_meta.at[pl.ds(0, 31)], zraw_meta.at[pl.ds(0, 15)]
    pltpu.make_async_copy(most, most, me_recv).wait()
    pltpu.make_async_copy(z_most, z_most, zm_recv).wait()
    lane = iota((1, BLK), 1)
    uses = (
        (got_meta, 8, SRC_ROWS, select, (0,)),
        (zraw_meta, 4, 2 * PLANE, zselect, (0, BLK)),
    )
    for metas, per, width, matrix, offsets in uses:
        for q in range(4):
            flat = jnp.zeros((1, BLK), f32)
            for n in range(per):
                at = (lane >= n * width) & (lane < (n + 1) * width)
                flat = jnp.where(at, metas[q * per + n], flat)
            for offset in offsets:
                row, col = iota((BLK, BLK), 0) + offset, iota((BLK, BLK), 1)
                fits = (row >> 4) == ((col & (width - 1)) >> 1)
                slot = ((row & (SLOTS - 1)) + 1).astype(f32)
                matrix[offset : offset + BLK, q * BLK : (q + 1) * BLK] = one_hot(
                    fits & (flat == slot)
                )

    def from_plane(k):
        f0, fn = SPLIT[k]
        chunk = pl.ds(f0, fn)
        arrived = got.at[chunk, all_but_own]
        pltpu.make_async_copy(arrived, arrived, pl_recv.at[k]).wait()
        for g in range(f0, f0 + fn):
            total = dot(select[...], got[g])
            own[g] = total[0:SLOTS]
            part[g] = total.astype(bf16)

        def send_z(dz, _):
            remote(
                part.at[chunk, pl.ds(pl.multiple_of(dz * SLOTS, SLOTS), SLOTS)],
                zgot.at[chunk, pl.ds(pl.multiple_of((dz - 1) * SLOTS, SLOTS), SLOTS)],
                z_send.at[k],
                z_recv.at[k],
                line_chip(dz),
                c,
            ).start()
            return 0

        lax.fori_loop(1, NZ, send_z, 0)

    for k in range(CHUNKS - 2):
        from_plane(k)

    pltpu.make_async_copy(zraw.at[:, z_but_own], zraw.at[:, z_but_own], zr_recv).wait()
    for g in range(ZN):
        total = dot(zselect[...], zraw[g])
        zown[g] = total[15 * SLOTS :]
        zpart[g] = total.astype(bf16)

    def send_sums(j, _):
        rows = pl.ds(pl.multiple_of((j - 1) * SLOTS, SLOTS), SLOTS)
        remote(
            zpart.at[:, rows], zlast.at[:, rows], zp_send, zp_recv, plane_chip(j), c
        ).start()
        return 0

    lax.fori_loop(1, PLANE, send_sums, 0)

    for k in range(CHUNKS - 2, CHUNKS):
        from_plane(k)

    def from_line(k):
        f0, fn = SPLIT[k]
        chunk = pl.ds(f0, fn)
        pltpu.make_async_copy(zgot.at[chunk], zgot.at[chunk], z_recv.at[k]).wait()
        for g in range(f0, f0 + fn):
            total = own[g]
            for s in range(NZ - 1):
                total = total + zgot[g, s * SLOTS : (s + 1) * SLOTS, :].astype(f32)
            last[g * OPITCH : g * OPITCH + SLOTS, :] = total

    for k in range(CHUNKS - 1):
        from_line(k)
    pltpu.make_async_copy(zlast, zlast, zp_recv).wait()
    for g in range(ZN):
        total = zown[g]
        for s in range(PLANE - 1):
            total = total + zlast[g, s * SLOTS : (s + 1) * SLOTS, :].astype(f32)
        last[(ZF + g) * OPITCH : (ZF + g) * OPITCH + SLOTS, :] = total
    from_line(CHUNKS - 1)
    last[HALF * OPITCH :, :] = jnp.zeros((OPITCH, BLK), jnp.float32)
    for s in range(SLOTS):
        line = last[pl.ds(s, 16, stride=OPITCH), :]
        out_ref[:, s * BLK : (s + 1) * BLK] = line[0:HALF]

    pltpu.make_async_copy(most, most, me_send).wait()
    pltpu.make_async_copy(z_most, z_most, zm_send).wait()
    pltpu.make_async_copy(zraw.at[:, z_but_own], zraw.at[:, z_but_own], zr_send).wait()
    pltpu.make_async_copy(zlast, zlast, zp_send).wait()
    for k in range(CHUNKS):
        chunk = pl.ds(*SPLIT[k])
        arrived = got.at[chunk, all_but_own]
        pltpu.make_async_copy(arrived, arrived, pl_send.at[k]).wait()
        pltpu.make_async_copy(zgot.at[chunk], zgot.at[chunk], z_send.at[k]).wait()


def local(ocean, grad_weight, neighbours, remap_weight, tile_src, tile_atm, atm_owner):
    bf16, f32, i32 = jnp.bfloat16, jnp.float32, jnp.int32
    vmem = pl.BlockSpec(memory_space=pltpu.VMEM)
    hbm = pl.BlockSpec(memory_space=pltpu.HBM)
    dma = pltpu.SemaphoreType.DMA
    return pl.pallas_call(
        kernel,
        out_shape=jax.ShapeDtypeStruct((HALF, NB * BLK), f32),
        in_specs=[hbm] * 7,
        out_specs=vmem,
        scratch_shapes=[
            pltpu.SMEM((4, NB), i32),
            pltpu.SMEM((1, TILES), i32),
            pltpu.VMEM((1, TILES), i32),
            pltpu.VMEM((NB, BLK), i32),
            pltpu.VMEM((2, HALF, EXT * BLK), bf16),
            pltpu.VMEM((EXT, 32, BLK), bf16),
            pltpu.VMEM((NB, 4 * BLK, 2 * BLK), bf16),
            pltpu.VMEM((TILES, 3 * BLK, BLK), bf16),
            pltpu.VMEM((NB, 32, 2 * BLK), bf16),
            pltpu.VMEM((TILES * PITCH, BLK), f32),
            pltpu.VMEM((2 * HALF, TILES, BLK), bf16),
            pltpu.VMEM((PLANE * SRC_ROWS, TILES), bf16),
            pltpu.VMEM((2 * HALF, PLANE * SRC_ROWS, BLK), bf16),
            pltpu.VMEM((PLANE, 1, BLK), f32),
            pltpu.VMEM((HALF, 32 * SRC_ROWS, BLK), bf16),
            pltpu.VMEM((32, 1, BLK), f32),
            pltpu.VMEM((NZ * SLOTS, 32 * SRC_ROWS), bf16),
            pltpu.VMEM((HALF, NZ * SLOTS, BLK), bf16),
            pltpu.VMEM((HALF, SLOTS, BLK), f32),
            pltpu.VMEM((HALF, (NZ - 1) * SLOTS, BLK), bf16),
            pltpu.VMEM((16 * OPITCH, BLK), f32),
            pltpu.VMEM((PLANE * SRC_ROWS, TILES), bf16),
            pltpu.VMEM((2 * ZN, PLANE * SRC_ROWS, BLK), bf16),
            pltpu.VMEM((NZ, 1, BLK), f32),
            pltpu.VMEM((ZN, 32 * SRC_ROWS, BLK), bf16),
            pltpu.VMEM((2 * NZ, 1, BLK), f32),
            pltpu.VMEM((PLANE * SLOTS, 32 * SRC_ROWS), bf16),
            pltpu.VMEM((ZN, PLANE * SLOTS, BLK), bf16),
            pltpu.VMEM((ZN, SLOTS, BLK), f32),
            pltpu.VMEM((ZN, (PLANE - 1) * SLOTS, BLK), bf16),
            dma((6,)),
            dma,
            dma((5,)),
            dma((5,)),
            pltpu.SemaphoreType.REGULAR,
            dma,
            dma,
            dma((CHUNKS,)),
            dma((CHUNKS,)),
            dma((CHUNKS,)),
            dma((CHUNKS,)),
            dma,
            dma,
            dma,
            dma,
            dma,
            dma,
        ],
        compiler_params=pltpu.CompilerParams(
            collective_id=0, has_side_effects=True, vmem_limit_bytes=48 * 1024 * 1024
        ),
    )(
        *(
            pltpu.with_memory_space_constraint(a, pltpu.HBM)
            for a in (
                ocean,
                grad_weight.reshape(NB, 4 * BLK, 2 * BLK),
                neighbours.T,
                remap_weight,
                tile_src[None, :],
                tile_atm[None, :],
                atm_owner.reshape(NB, BLK),
            )
        )
    )


def solution(mesh):
    in_specs = (
        P("field", "dom"),
        P("dom", None, None, None),
        P("dom", None),
        P(("dom", "field"), None, None),
        P(("dom", "field")),
        P(("dom", "field")),
        P(),
    )
    out_specs = P("field", "dom")
    return jax.shard_map(local, mesh=mesh, in_specs=in_specs, out_specs=out_specs, check_vma=False)
```

```python
import functools

import jax
import jax.numpy as jnp
from jax import lax
from jax.experimental import pallas as pl
from jax.experimental.pallas import tpu as pltpu
from jax.sharding import PartitionSpec as P

MESH = pl.DeviceIdType.MESH
NX, NZ, NY = 4, 8, 4
PLANE = NX * NY
HALF = 15
BLK = 128
NB = 16
NH = 2
EXT = NB + 2 * NH
TILES = 64
SLOTS = 16
SRC_ROWS = 16
SPLIT = ((0, 3), (3, 3), (6, 3), (9, 2), (11, 1))
CHUNKS = len(SPLIT)
ZF, ZN = 12, 3
PITCH = 40
OPITCH = 24


def coords():
    d = lax.axis_index("dom")
    return lax.div(d, NZ * NY), lax.rem(lax.div(d, NY), NZ), lax.rem(d, NY)


def chip(x, z, y):
    return (x * NZ + z) * NY + y


def kernel(
    ocean_hbm,
    gw_hbm,
    nb_hbm,
    rw_hbm,
    src_hbm,
    atm_hbm,
    owner_hbm,
    out_ref,
    nb_ref,
    src_ref,
    atm,
    owners,
    raw,
    relay,
    wide,
    gw,
    rw,
    grads,
    cont,
    fields,
    pack,
    sent,
    sent_meta,
    got,
    got_meta,
    select,
    part,
    own,
    zgot,
    last,
    zpack,
    zsent,
    zsent_meta,
    zraw,
    zraw_meta,
    zselect,
    zpart,
    zown,
    zlast,
    load_sem,
    w_sem,
    oc_send,
    oc_recv,
    near_sem,
    me_send,
    me_recv,
    pl_send,
    pl_recv,
    z_send,
    z_recv,
    zm_send,
    zm_recv,
    zr_send,
    zr_recv,
    zp_send,
    zp_recv,
):
    c = lax.axis_index("field")
    d = lax.axis_index("dom")
    x, z, y = coords()
    other = 1 - c
    devices = NX * NZ * NY
    up, down = lax.rem(d + 1, devices), lax.rem(d + devices - 1, devices)

    def plane_chip(j):
        return chip(lax.rem(x + lax.div(j, NY), NX), z, lax.rem(y + lax.rem(j, NY), NY))

    def line_chip(dz):
        return chip(x, lax.rem(z + dz, NZ), y)

    ocean_in = pltpu.make_async_copy(
        ocean_hbm, raw.at[c, :, pl.ds(NH * BLK, NB * BLK)], load_sem.at[0]
    )
    ocean_in.start()
    small = [
        pltpu.make_async_copy(src, dst, load_sem.at[n])
        for n, (src, dst) in enumerate(
            ((atm_hbm, atm), (owner_hbm, owners), (nb_hbm, nb_ref), (src_hbm, src_ref)), 1
        )
    ]
    for copy in small:
        copy.start()
    gw_in = pltpu.make_async_copy(gw_hbm, gw, load_sem.at[5])
    gw_in.start()
    rw_in = pltpu.make_async_copy(rw_hbm, rw, w_sem)
    rw_in.start()

    barrier = pltpu.get_barrier_semaphore()

    def greet(dom, core, sem=barrier):
        pl.semaphore_signal(
            sem, inc=1, device_id={"dom": dom, "field": core}, device_id_type=MESH
        )

    y_ring = [chip(x, z, lax.rem(y + n, NY)) for n in range(1, NY)]
    ahead = chip(lax.rem(x + 1, NX), z, lax.rem(y + 1, NY))
    behind = chip(lax.rem(x + NX - 1, NX), z, lax.rem(y + NY - 1, NY))
    z_near = [chip(x, lax.rem(z + n, NZ), y) for n in (1, NZ - 1, 2, NZ - 2)]
    for h in range(2):
        greet(up, h)
        greet(down, h)
    for dom in z_near:
        greet(dom, 0)
        greet(dom, 1)
    for dom in y_ring:
        greet(dom, c)
    for n in range(1, NX):
        for h in range(2):
            greet(chip(lax.rem(x + n, NX), z, y), h)
    greet(ahead, c)
    greet(behind, c)
    greet(d, other)

    small[0].wait()
    small[1].wait()
    bf16, f32 = jnp.bfloat16, jnp.float32

    def dot(a, b):
        return jnp.dot(a, b, preferred_element_type=f32)

    def iota(shape, dim):
        return lax.broadcasted_iota(jnp.int32, shape, dim)

    def one_hot(mask):
        return jnp.where(mask, 1.0, 0.0).astype(bf16)

    ids = atm[...]
    table = owners[...]
    halves = jnp.concatenate([table >> 4, table & 15], axis=0).astype(f32).astype(bf16)
    found = dot(halves, one_hot(iota((BLK, TILES), 0) == (ids & (BLK - 1))))
    here = iota((16, TILES), 0) == (ids >> 7)
    owner_row = jnp.sum(jnp.where(here, found[0:16], 0.0), axis=0, keepdims=True)
    slot_row = jnp.sum(jnp.where(here, found[16:32], 0.0), axis=0, keepdims=True)
    square = (TILES, TILES)
    diagonal = jnp.where(iota(square, 0) == iota(square, 1), owner_row, 0.0).astype(bf16)
    owner_col = dot(diagonal, jnp.ones(square, bf16))
    earlier = (owner_col == owner_row) & (iota(square, 0) < iota(square, 1))
    rank = jnp.sum(jnp.where(earlier, 1, 0), axis=0, keepdims=True)
    owner = owner_row.astype(jnp.int32)
    dx = ((owner >> 5) - x) & (NX - 1)
    dz = ((owner >> 2) - z) & (NZ - 1)
    dy = (owner - y) & (NY - 1)
    jj = (dx * NY + dy + PLANE - 1) & (PLANE - 1)
    z_rel = (dz + NZ - 1) & (NZ - 1)
    within = (dz * 2 + rank, jj * 2 + rank)
    plans = (
        (jj, within[0], SRC_ROWS, pack, sent_meta),
        (z_rel, within[1], 2 * PLANE, zpack, zsent_meta),
    )
    for group, inner, width, matrix, metas in plans:
        matrix[...] = one_hot(iota((PLANE * SRC_ROWS, TILES), 0) == group * width + inner)
        marked = jnp.where(iota((PLANE, TILES), 0) == group, slot_row + 1.0, 0.0).astype(bf16)
        spread = jnp.where(iota(square, 0) == iota(square, 1), inner.astype(f32), 0.0)
        inner_col = dot(spread.astype(bf16), jnp.ones((TILES, BLK), bf16))
        lanes = (iota((TILES, BLK), 1) & (width - 1)).astype(f32)
        table = dot(marked, one_hot(inner_col == lanes))
        for n in range(metas.shape[0]):
            metas[n] = table[n : n + 1]
    ocean_in.wait()

    pl.semaphore_wait(barrier, 4 + 8 + 3 + 6 + 2 + 1)

    def remote(src, dst, send, recv, dom, core):
        return pltpu.make_async_remote_copy(
            src_ref=src,
            dst_ref=dst,
            send_sem=send,
            recv_sem=recv,
            device_id={"dom": dom, "field": core},
            device_id_type=MESH,
        )

    first = pl.ds(NH * BLK, NH * BLK)
    final = pl.ds(NB * BLK, NH * BLK)
    left = pl.ds(0, NH * BLK)
    right = pl.ds((NB + NH) * BLK, NH * BLK)
    middle = pl.ds(NH * BLK, NB * BLK)
    half = raw.at[c]
    upward = [
        remote(half.at[:, final], half.at[:, left], oc_send.at[n], oc_recv.at[n], up, h)
        for n, h in enumerate((c, other))
    ]
    downward = [
        remote(half.at[:, first], half.at[:, right], oc_send.at[2 + n], oc_recv.at[2 + n], down, h)
        for n, h in enumerate((c, other))
    ]
    sideways = remote(
        half.at[:, middle], half.at[:, middle], oc_send.at[4], oc_recv.at[4], d, other
    )
    to_relay = remote(half.at[:, first], relay, oc_send.at[5], oc_recv.at[5], behind, c)
    below = chip(x, NZ - 1, y)
    relayed = [
        remote(relay, half.at[:, right], oc_send.at[6 + n], oc_recv.at[2 + n], below, h)
        for n, h in enumerate((c, other))
    ]
    corner = (z == 0) & (y == 0)
    relaying = (z == 0) & (y == NY - 1)
    for copy in upward:
        copy.start()

    @pl.when(corner)
    def _():
        to_relay.start()

    @pl.when(jnp.logical_not(corner))
    def _():
        for copy in downward:
            copy.start()

    sideways.start()
    for dom in y_ring + z_near[2:]:
        greet(dom, c, near_sem)
    @pl.when(relaying)
    def _():
        to_relay.wait_recv()
        for copy in relayed:
            copy.start()

    sideways.wait_recv()
    wide[...] = jnp.zeros_like(wide)

    def spread_blocks(blocks):
        for e in blocks:
            wide[e, 0:HALF, :] = raw[0, :, e * BLK : (e + 1) * BLK]
            wide[e, 16 : 16 + HALF, :] = raw[1, :, e * BLK : (e + 1) * BLK]

    spread_blocks(range(NH, NH + NB))
    small[2].wait()
    small[3].wait()
    rw_in.wait()
    own_block = d * NB

    def remap_values(t, _):
        s = jnp.maximum(src_ref[0, t] - own_block, 0)
        cont[pl.ds(pl.multiple_of(t * PITCH, 8), 32), :] = dot(wide[s + NH], rw[t, 0:BLK, :])
        return 0

    lax.fori_loop(0, TILES, remap_values, 0, unroll=8)
    for copy in upward + downward:
        copy.wait_recv()
    spread_blocks((0, 1, NH + NB, NH + NB + 1))

    gw_in.wait()

    first_block = d * NB - NH

    def gradient(b, _):
        picked = jnp.concatenate(
            [wide[jnp.maximum(nb_ref[k, b] - first_block, 0)] for k in range(4)], axis=1
        )
        grads[b] = jnp.dot(picked, gw[b], preferred_element_type=jnp.float32).astype(
            jnp.bfloat16
        )
        return 0

    lax.fori_loop(0, NB, gradient, 0, unroll=4)
    def remap(t, _):
        s = jnp.maximum(src_ref[0, t] - own_block, 0)
        at = pl.ds(pl.multiple_of(t * PITCH, 8), 32)
        cont[at, :] = cont[at, :] + dot(grads[s], rw[t, BLK:, :])
        return 0

    lax.fori_loop(0, TILES, remap, 0, unroll=8)

    def turn(g, _):
        for h in range(2):
            fields[h * HALF + g] = cont[pl.ds(h * 16 + g, TILES, stride=PITCH), :].astype(
                jnp.bfloat16
            )
        return 0

    pl.semaphore_wait(near_sem, 5)

    remote(sent_meta.at[15], got_meta.at[30], me_send, me_recv, d, other).start()
    remote(zsent_meta.at[7], zraw_meta.at[14], zm_send, zm_recv, d, other).start()

    def send_meta(j, _):
        for h in range(2):
            remote(
                sent_meta.at[j - 1],
                got_meta.at[(j - 1) * 2 + c],
                me_send,
                me_recv,
                plane_chip(j),
                h,
            ).start()
        return 0

    def send_zmeta(dz, _):
        for h in range(2):
            remote(
                zsent_meta.at[dz - 1],
                zraw_meta.at[(dz - 1) * 2 + c],
                zm_send,
                zm_recv,
                line_chip(dz),
                h,
            ).start()
        return 0

    lax.fori_loop(1, PLANE, send_meta, 0)
    lax.fori_loop(1, NZ, send_zmeta, 0)
    got_meta[31] = sent_meta[15]
    zraw_meta[15] = zsent_meta[7]

    def z_rows(start):
        return pl.ds(pl.multiple_of(start * 32, 32), 32)

    own_rows = pl.ds(15 * SRC_ROWS, SRC_ROWS)
    all_but_own = pl.ds(0, 31 * SRC_ROWS)
    z_but_own = pl.ds(0, 15 * 32)
    zchunk = pl.ds(ZF, ZN)

    def send_plane(k):
        f0, fn = SPLIT[k]
        for g in range(f0, f0 + fn):
            turn(g, 0)
        for h in range(2):
            for g in range(f0, f0 + fn):
                f = h * HALF + g
                sent[f] = dot(pack[...], fields[f]).astype(bf16)
        chunk = pl.ds(f0, fn)
        remote(
            sent.at[pl.ds(other * HALF + f0, fn), own_rows],
            got.at[chunk, pl.ds(30 * SRC_ROWS, SRC_ROWS)],
            pl_send.at[k],
            pl_recv.at[k],
            d,
            other,
        ).start()

        def send(j, _):
            dom = plane_chip(j)
            for h in range(2):
                remote(
                    sent.at[
                        pl.ds(h * HALF + f0, fn),
                        pl.ds(pl.multiple_of((j - 1) * SRC_ROWS, SRC_ROWS), SRC_ROWS),
                    ],
                    got.at[
                        chunk,
                        pl.ds(pl.multiple_of(((j - 1) * 2 + c) * SRC_ROWS, SRC_ROWS), SRC_ROWS),
                    ],
                    pl_send.at[k],
                    pl_recv.at[k],
                    dom,
                    h,
                ).start()
            return 0

        lax.fori_loop(1, PLANE, send, 0)
        got[chunk, pl.ds(31 * SRC_ROWS, SRC_ROWS), :] = sent[
            pl.ds(c * HALF + f0, fn), own_rows, :
        ]

    send_plane(0)
    for g in range(ZF, ZF + ZN):
        turn(g, 0)
    for h in range(2):
        for g in range(ZN):
            zsent[h * ZN + g] = dot(zpack[...], fields[h * HALF + ZF + g]).astype(bf16)
    remote(
        zsent.at[pl.ds(other * ZN, ZN), z_rows(7)],
        zraw.at[:, z_rows(14)],
        zr_send,
        zr_recv,
        d,
        other,
    ).start()

    def send_raw(dz, _):
        for h in range(2):
            remote(
                zsent.at[pl.ds(h * ZN, ZN), z_rows(dz - 1)],
                zraw.at[:, z_rows((dz - 1) * 2 + c)],
                zr_send,
                zr_recv,
                line_chip(dz),
                h,
            ).start()
        return 0

    lax.fori_loop(1, NZ, send_raw, 0)
    zraw[:, z_rows(15), :] = zsent[pl.ds(c * ZN, ZN), z_rows(7), :]
    for k in range(1, CHUNKS):
        send_plane(k)

    most, z_most = got_meta.at[pl.ds(0, 31)], zraw_meta.at[pl.ds(0, 15)]
    pltpu.make_async_copy(most, most, me_recv).wait()
    pltpu.make_async_copy(z_most, z_most, zm_recv).wait()
    lane = iota((1, BLK), 1)
    uses = (
        (got_meta, 8, SRC_ROWS, select, (0,)),
        (zraw_meta, 4, 2 * PLANE, zselect, (0, BLK)),
    )
    for metas, per, width, matrix, offsets in uses:
        for q in range(4):
            flat = jnp.zeros((1, BLK), f32)
            for n in range(per):
                at = (lane >= n * width) & (lane < (n + 1) * width)
                flat = jnp.where(at, metas[q * per + n], flat)
            for offset in offsets:
                row, col = iota((BLK, BLK), 0) + offset, iota((BLK, BLK), 1)
                fits = (row >> 4) == ((col & (width - 1)) >> 1)
                slot = ((row & (SLOTS - 1)) + 1).astype(f32)
                matrix[offset : offset + BLK, q * BLK : (q + 1) * BLK] = one_hot(
                    fits & (flat == slot)
                )

    def from_plane(k):
        f0, fn = SPLIT[k]
        chunk = pl.ds(f0, fn)
        arrived = got.at[chunk, all_but_own]
        pltpu.make_async_copy(arrived, arrived, pl_recv.at[k]).wait()
        for g in range(f0, f0 + fn):
            total = dot(select[...], got[g])
            own[g] = total[0:SLOTS]
            part[g] = total.astype(bf16)

        def send_z(dz, _):
            remote(
                part.at[chunk, pl.ds(pl.multiple_of(dz * SLOTS, SLOTS), SLOTS)],
                zgot.at[chunk, pl.ds(pl.multiple_of((dz - 1) * SLOTS, SLOTS), SLOTS)],
                z_send.at[k],
                z_recv.at[k],
                line_chip(dz),
                c,
            ).start()
            return 0

        lax.fori_loop(1, NZ, send_z, 0)

    for k in range(CHUNKS - 2):
        from_plane(k)

    pltpu.make_async_copy(zraw.at[:, z_but_own], zraw.at[:, z_but_own], zr_recv).wait()
    for g in range(ZN):
        total = dot(zselect[...], zraw[g])
        zown[g] = total[15 * SLOTS :]
        zpart[g] = total.astype(bf16)

    def send_sums(j, _):
        rows = pl.ds(pl.multiple_of((j - 1) * SLOTS, SLOTS), SLOTS)
        remote(
            zpart.at[:, rows], zlast.at[:, rows], zp_send, zp_recv, plane_chip(j), c
        ).start()
        return 0

    lax.fori_loop(1, PLANE, send_sums, 0)

    for k in range(CHUNKS - 2, CHUNKS):
        from_plane(k)

    def from_line(k):
        f0, fn = SPLIT[k]
        chunk = pl.ds(f0, fn)
        pltpu.make_async_copy(zgot.at[chunk], zgot.at[chunk], z_recv.at[k]).wait()
        for g in range(f0, f0 + fn):
            total = own[g]
            for s in range(NZ - 1):
                total = total + zgot[g, s * SLOTS : (s + 1) * SLOTS, :].astype(f32)
            last[g * OPITCH : g * OPITCH + SLOTS, :] = total

    for k in range(CHUNKS - 1):
        from_line(k)
    pltpu.make_async_copy(zlast, zlast, zp_recv).wait()
    for g in range(ZN):
        total = zown[g]
        for s in range(PLANE - 1):
            total = total + zlast[g, s * SLOTS : (s + 1) * SLOTS, :].astype(f32)
        last[(ZF + g) * OPITCH : (ZF + g) * OPITCH + SLOTS, :] = total
    from_line(CHUNKS - 1)
    last[HALF * OPITCH :, :] = jnp.zeros((OPITCH, BLK), jnp.float32)
    for s in range(SLOTS):
        line = last[pl.ds(s, 16, stride=OPITCH), :]
        out_ref[:, s * BLK : (s + 1) * BLK] = line[0:HALF]

    for copy in upward:
        copy.wait_send()
    sideways.wait_send()

    @pl.when(corner)
    def _():
        to_relay.wait_send()

    @pl.when(jnp.logical_not(corner))
    def _():
        for copy in downward:
            copy.wait_send()

    @pl.when(relaying)
    def _():
        for copy in relayed:
            copy.wait_send()

    pltpu.make_async_copy(most, most, me_send).wait()
    pltpu.make_async_copy(z_most, z_most, zm_send).wait()
    pltpu.make_async_copy(zraw.at[:, z_but_own], zraw.at[:, z_but_own], zr_send).wait()
    pltpu.make_async_copy(zlast, zlast, zp_send).wait()
    for k in range(CHUNKS):
        chunk = pl.ds(*SPLIT[k])
        arrived = got.at[chunk, all_but_own]
        pltpu.make_async_copy(arrived, arrived, pl_send.at[k]).wait()
        pltpu.make_async_copy(zgot.at[chunk], zgot.at[chunk], z_send.at[k]).wait()


def local(ocean, grad_weight, neighbours, remap_weight, tile_src, tile_atm, atm_owner):
    bf16, f32, i32 = jnp.bfloat16, jnp.float32, jnp.int32
    vmem = pl.BlockSpec(memory_space=pltpu.VMEM)
    hbm = pl.BlockSpec(memory_space=pltpu.HBM)
    dma = pltpu.SemaphoreType.DMA
    return pl.pallas_call(
        kernel,
        out_shape=jax.ShapeDtypeStruct((HALF, NB * BLK), f32),
        in_specs=[hbm] * 7,
        out_specs=vmem,
        scratch_shapes=[
            pltpu.SMEM((4, NB), i32),
            pltpu.SMEM((1, TILES), i32),
            pltpu.VMEM((1, TILES), i32),
            pltpu.VMEM((NB, BLK), i32),
            pltpu.VMEM((2, HALF, EXT * BLK), bf16),
            pltpu.VMEM((HALF, NH * BLK), bf16),
            pltpu.VMEM((EXT, 32, BLK), bf16),
            pltpu.VMEM((NB, 4 * BLK, 2 * BLK), bf16),
            pltpu.VMEM((TILES, 3 * BLK, BLK), bf16),
            pltpu.VMEM((NB, 32, 2 * BLK), bf16),
            pltpu.VMEM((TILES * PITCH, BLK), f32),
            pltpu.VMEM((2 * HALF, TILES, BLK), bf16),
            pltpu.VMEM((PLANE * SRC_ROWS, TILES), bf16),
            pltpu.VMEM((2 * HALF, PLANE * SRC_ROWS, BLK), bf16),
            pltpu.VMEM((PLANE, 1, BLK), f32),
            pltpu.VMEM((HALF, 32 * SRC_ROWS, BLK), bf16),
            pltpu.VMEM((32, 1, BLK), f32),
            pltpu.VMEM((NZ * SLOTS, 32 * SRC_ROWS), bf16),
            pltpu.VMEM((HALF, NZ * SLOTS, BLK), bf16),
            pltpu.VMEM((HALF, SLOTS, BLK), f32),
            pltpu.VMEM((HALF, (NZ - 1) * SLOTS, BLK), bf16),
            pltpu.VMEM((16 * OPITCH, BLK), f32),
            pltpu.VMEM((PLANE * SRC_ROWS, TILES), bf16),
            pltpu.VMEM((2 * ZN, PLANE * SRC_ROWS, BLK), bf16),
            pltpu.VMEM((NZ, 1, BLK), f32),
            pltpu.VMEM((ZN, 32 * SRC_ROWS, BLK), bf16),
            pltpu.VMEM((2 * NZ, 1, BLK), f32),
            pltpu.VMEM((PLANE * SLOTS, 32 * SRC_ROWS), bf16),
            pltpu.VMEM((ZN, PLANE * SLOTS, BLK), bf16),
            pltpu.VMEM((ZN, SLOTS, BLK), f32),
            pltpu.VMEM((ZN, (PLANE - 1) * SLOTS, BLK), bf16),
            dma((6,)),
            dma,
            dma((8,)),
            dma((6,)),
            pltpu.SemaphoreType.REGULAR,
            dma,
            dma,
            dma((CHUNKS,)),
            dma((CHUNKS,)),
            dma((CHUNKS,)),
            dma((CHUNKS,)),
            dma,
            dma,
            dma,
            dma,
            dma,
            dma,
        ],
        compiler_params=pltpu.CompilerParams(
            collective_id=0, has_side_effects=True, vmem_limit_bytes=48 * 1024 * 1024
        ),
    )(
        *(
            pltpu.with_memory_space_constraint(a, pltpu.HBM)
            for a in (
                ocean,
                grad_weight.reshape(NB, 4 * BLK, 2 * BLK),
                neighbours.T,
                remap_weight,
                tile_src[None, :],
                tile_atm[None, :],
                atm_owner.reshape(NB, BLK),
            )
        )
    )


def solution(mesh):
    in_specs = (
        P("field", "dom"),
        P("dom", None, None, None),
        P("dom", None),
        P(("dom", "field"), None, None),
        P(("dom", "field")),
        P(("dom", "field")),
        P(),
    )
    out_specs = P("field", "dom")
    return jax.shard_map(local, mesh=mesh, in_specs=in_specs, out_specs=out_specs, check_vma=False)
```

```python
import functools

import jax
import jax.numpy as jnp
from jax import lax
from jax.experimental import pallas as pl
from jax.experimental.pallas import tpu as pltpu
from jax.sharding import PartitionSpec as P

MESH = pl.DeviceIdType.MESH
NX, NZ, NY = 4, 8, 4
PLANE = NX * NY
HALF = 15
BLK = 128
NB = 16
NH = 2
EXT = NB + 2 * NH
TILES = 64
SLOTS = 16
SRC_ROWS = 16
SPLIT = ((0, 3), (3, 3), (6, 2), (8, 2), (10, 1))
CHUNKS = len(SPLIT)
ZF, ZN = 11, 4
PITCH = 40
OPITCH = 24


def coords():
    d = lax.axis_index("dom")
    return lax.div(d, NZ * NY), lax.rem(lax.div(d, NY), NZ), lax.rem(d, NY)


def chip(x, z, y):
    return (x * NZ + z) * NY + y


def kernel(
    ocean_hbm,
    gw_hbm,
    nb_hbm,
    rw_hbm,
    src_hbm,
    atm_hbm,
    owner_hbm,
    out_ref,
    nb_ref,
    src_ref,
    atm,
    owners,
    raw,
    relay,
    wide,
    gw,
    rw,
    grads,
    cont,
    fields,
    pack,
    sent,
    sent_meta,
    got,
    got_meta,
    select,
    part,
    own,
    zgot,
    last,
    zpack,
    zsent,
    zsent_meta,
    zraw,
    zraw_meta,
    zselect,
    zpart,
    zown,
    zlast,
    load_sem,
    w_sem,
    oc_send,
    oc_recv,
    near_sem,
    me_send,
    me_recv,
    pl_send,
    pl_recv,
    z_send,
    z_recv,
    zm_send,
    zm_recv,
    zr_send,
    zr_recv,
    zp_send,
    zp_recv,
):
    c = lax.axis_index("field")
    d = lax.axis_index("dom")
    x, z, y = coords()
    other = 1 - c
    devices = NX * NZ * NY
    up, down = lax.rem(d + 1, devices), lax.rem(d + devices - 1, devices)

    def plane_chip(j):
        return chip(lax.rem(x + lax.div(j, NY), NX), z, lax.rem(y + lax.rem(j, NY), NY))

    def line_chip(dz):
        return chip(x, lax.rem(z + dz, NZ), y)

    ocean_in = pltpu.make_async_copy(
        ocean_hbm, raw.at[c, :, pl.ds(NH * BLK, NB * BLK)], load_sem.at[0]
    )
    ocean_in.start()
    small = [
        pltpu.make_async_copy(src, dst, load_sem.at[n])
        for n, (src, dst) in enumerate(
            ((atm_hbm, atm), (owner_hbm, owners), (nb_hbm, nb_ref), (src_hbm, src_ref)), 1
        )
    ]
    for copy in small:
        copy.start()
    gw_in = pltpu.make_async_copy(gw_hbm, gw, load_sem.at[5])
    gw_in.start()
    rw_in = pltpu.make_async_copy(rw_hbm, rw, w_sem)
    rw_in.start()

    barrier = pltpu.get_barrier_semaphore()

    def greet(dom, core, sem=barrier):
        pl.semaphore_signal(
            sem, inc=1, device_id={"dom": dom, "field": core}, device_id_type=MESH
        )

    y_ring = [chip(x, z, lax.rem(y + n, NY)) for n in range(1, NY)]
    ahead = chip(lax.rem(x + 1, NX), z, lax.rem(y + 1, NY))
    behind = chip(lax.rem(x + NX - 1, NX), z, lax.rem(y + NY - 1, NY))
    z_near = [chip(x, lax.rem(z + n, NZ), y) for n in (1, NZ - 1, 2, NZ - 2)]
    corner = (z == 0) & (y == 0)
    relaying = (z == 0) & (y == NY - 1)

    @pl.when(jnp.logical_not((z == NZ - 1) & (y == NY - 1)))
    def _():
        greet(up, 0)
        greet(up, 1)

    greet(down, 0)
    greet(down, 1)
    for dom in z_near:
        greet(dom, 0)
        greet(dom, 1)
    for dom in y_ring:
        greet(dom, c)
    for n in range(1, NX):
        for h in range(2):
            greet(chip(lax.rem(x + n, NX), z, y), h)
    greet(ahead, c)
    greet(behind, c)
    greet(d, other)

    small[0].wait()
    small[1].wait()
    bf16, f32 = jnp.bfloat16, jnp.float32

    def dot(a, b):
        return jnp.dot(a, b, preferred_element_type=f32)

    def iota(shape, dim):
        return lax.broadcasted_iota(jnp.int32, shape, dim)

    def one_hot(mask):
        return jnp.where(mask, 1.0, 0.0).astype(bf16)

    ids = atm[...]
    table = owners[...]
    halves = jnp.concatenate([table >> 4, table & 15], axis=0).astype(f32).astype(bf16)
    found = dot(halves, one_hot(iota((BLK, TILES), 0) == (ids & (BLK - 1))))
    here = iota((16, TILES), 0) == (ids >> 7)
    owner_row = jnp.sum(jnp.where(here, found[0:16], 0.0), axis=0, keepdims=True)
    slot_row = jnp.sum(jnp.where(here, found[16:32], 0.0), axis=0, keepdims=True)
    square = (TILES, TILES)
    diagonal = jnp.where(iota(square, 0) == iota(square, 1), owner_row, 0.0).astype(bf16)
    owner_col = dot(diagonal, jnp.ones(square, bf16))
    earlier = (owner_col == owner_row) & (iota(square, 0) < iota(square, 1))
    rank = jnp.sum(jnp.where(earlier, 1, 0), axis=0, keepdims=True)
    owner = owner_row.astype(jnp.int32)
    dx = ((owner >> 5) - x) & (NX - 1)
    dz = ((owner >> 2) - z) & (NZ - 1)
    dy = (owner - y) & (NY - 1)
    jj = (dx * NY + dy + PLANE - 1) & (PLANE - 1)
    z_rel = (dz + NZ - 1) & (NZ - 1)
    within = (dz * 2 + rank, jj * 2 + rank)
    plans = (
        (jj, within[0], SRC_ROWS, pack, sent_meta),
        (z_rel, within[1], 2 * PLANE, zpack, zsent_meta),
    )
    for group, inner, width, matrix, metas in plans:
        matrix[...] = one_hot(iota((PLANE * SRC_ROWS, TILES), 0) == group * width + inner)
        marked = jnp.where(iota((PLANE, TILES), 0) == group, slot_row + 1.0, 0.0).astype(bf16)
        spread = jnp.where(iota(square, 0) == iota(square, 1), inner.astype(f32), 0.0)
        inner_col = dot(spread.astype(bf16), jnp.ones((TILES, BLK), bf16))
        lanes = (iota((TILES, BLK), 1) & (width - 1)).astype(f32)
        table = dot(marked, one_hot(inner_col == lanes))
        for n in range(metas.shape[0]):
            metas[n] = table[n : n + 1]
    ocean_in.wait()

    pl.semaphore_wait(barrier, jnp.where(corner, 2, 4) + 8 + 3 + 6 + 2 + 1)

    def remote(src, dst, send, recv, dom, core):
        return pltpu.make_async_remote_copy(
            src_ref=src,
            dst_ref=dst,
            send_sem=send,
            recv_sem=recv,
            device_id={"dom": dom, "field": core},
            device_id_type=MESH,
        )

    first = pl.ds(NH * BLK, NH * BLK)
    final = pl.ds(NB * BLK, NH * BLK)
    left = pl.ds(0, NH * BLK)
    right = pl.ds((NB + NH) * BLK, NH * BLK)
    middle = pl.ds(NH * BLK, NB * BLK)
    half = raw.at[c]
    upward = [
        remote(half.at[:, final], half.at[:, left], oc_send.at[n], oc_recv.at[n], up, h)
        for n, h in enumerate((c, other))
    ]
    downward = [
        remote(half.at[:, first], half.at[:, right], oc_send.at[2 + n], oc_recv.at[2 + n], down, h)
        for n, h in enumerate((c, other))
    ]
    sideways = remote(
        half.at[:, middle], half.at[:, middle], oc_send.at[4], oc_recv.at[4], d, other
    )
    to_relay = remote(half.at[:, first], relay, oc_send.at[5], oc_recv.at[5], behind, c)
    below = chip(x, NZ - 1, y)
    relayed = [
        remote(relay, half.at[:, right], oc_send.at[6 + n], oc_recv.at[2 + n], below, h)
        for n, h in enumerate((c, other))
    ]
    for copy in upward:
        copy.start()

    @pl.when(corner)
    def _():
        to_relay.start()

    @pl.when(jnp.logical_not(corner))
    def _():
        for copy in downward:
            copy.start()

    sideways.start()
    for dom in y_ring + z_near[2:]:
        greet(dom, c, near_sem)
    @pl.when(relaying)
    def _():
        to_relay.wait_recv()
        for copy in relayed:
            copy.start()

    sideways.wait_recv()
    wide[...] = jnp.zeros_like(wide)

    def spread_blocks(blocks):
        for e in blocks:
            wide[e, 0:HALF, :] = raw[0, :, e * BLK : (e + 1) * BLK]
            wide[e, 16 : 16 + HALF, :] = raw[1, :, e * BLK : (e + 1) * BLK]

    spread_blocks(range(NH, NH + NB))
    small[2].wait()
    small[3].wait()
    rw_in.wait()
    own_block = d * NB

    def remap_values(t, _):
        s = jnp.maximum(src_ref[0, t] - own_block, 0)
        cont[pl.ds(pl.multiple_of(t * PITCH, 8), 32), :] = dot(wide[s + NH], rw[t, 0:BLK, :])
        return 0

    lax.fori_loop(0, TILES, remap_values, 0, unroll=8)
    for copy in upward + downward:
        copy.wait_recv()
    spread_blocks((0, 1, NH + NB, NH + NB + 1))

    gw_in.wait()

    first_block = d * NB - NH

    def gradient(b, _):
        picked = jnp.concatenate(
            [wide[jnp.maximum(nb_ref[k, b] - first_block, 0)] for k in range(4)], axis=1
        )
        grads[b] = jnp.dot(picked, gw[b], preferred_element_type=jnp.float32).astype(
            jnp.bfloat16
        )
        return 0

    lax.fori_loop(0, NB, gradient, 0, unroll=4)
    def remap(t, _):
        s = jnp.maximum(src_ref[0, t] - own_block, 0)
        at = pl.ds(pl.multiple_of(t * PITCH, 8), 32)
        cont[at, :] = cont[at, :] + dot(grads[s], rw[t, BLK:, :])
        return 0

    lax.fori_loop(0, TILES, remap, 0, unroll=8)

    def turn(g, _):
        for h in range(2):
            fields[h * HALF + g] = cont[pl.ds(h * 16 + g, TILES, stride=PITCH), :].astype(
                jnp.bfloat16
            )
        return 0

    pl.semaphore_wait(near_sem, 5)

    def z_rows(start):
        return pl.ds(pl.multiple_of(start * 32, 32), 32)

    own_rows = pl.ds(15 * SRC_ROWS, SRC_ROWS)
    all_but_own = pl.ds(0, 31 * SRC_ROWS)
    z_but_own = pl.ds(0, 15 * 32)
    zchunk = pl.ds(ZF, ZN)

    def send_plane(k):
        f0, fn = SPLIT[k]
        for g in range(f0, f0 + fn):
            turn(g, 0)
        for h in range(2):
            for g in range(f0, f0 + fn):
                f = h * HALF + g
                sent[f] = dot(pack[...], fields[f]).astype(bf16)
        chunk = pl.ds(f0, fn)
        remote(
            sent.at[pl.ds(other * HALF + f0, fn), own_rows],
            got.at[chunk, pl.ds(30 * SRC_ROWS, SRC_ROWS)],
            pl_send.at[k],
            pl_recv.at[k],
            d,
            other,
        ).start()

        def send(j, _):
            dom = plane_chip(j)
            for h in range(2):
                remote(
                    sent.at[
                        pl.ds(h * HALF + f0, fn),
                        pl.ds(pl.multiple_of((j - 1) * SRC_ROWS, SRC_ROWS), SRC_ROWS),
                    ],
                    got.at[
                        chunk,
                        pl.ds(pl.multiple_of(((j - 1) * 2 + c) * SRC_ROWS, SRC_ROWS), SRC_ROWS),
                    ],
                    pl_send.at[k],
                    pl_recv.at[k],
                    dom,
                    h,
                ).start()
            return 0

        lax.fori_loop(1, PLANE, send, 0)
        got[chunk, pl.ds(31 * SRC_ROWS, SRC_ROWS), :] = sent[
            pl.ds(c * HALF + f0, fn), own_rows, :
        ]

    send_plane(0)
    remote(sent_meta.at[15], got_meta.at[30], me_send, me_recv, d, other).start()
    remote(zsent_meta.at[7], zraw_meta.at[14], zm_send, zm_recv, d, other).start()

    def send_meta(j, _):
        for h in range(2):
            remote(
                sent_meta.at[j - 1],
                got_meta.at[(j - 1) * 2 + c],
                me_send,
                me_recv,
                plane_chip(j),
                h,
            ).start()
        return 0

    def send_zmeta(dz, _):
        for h in range(2):
            remote(
                zsent_meta.at[dz - 1],
                zraw_meta.at[(dz - 1) * 2 + c],
                zm_send,
                zm_recv,
                line_chip(dz),
                h,
            ).start()
        return 0

    lax.fori_loop(1, PLANE, send_meta, 0)
    lax.fori_loop(1, NZ, send_zmeta, 0)
    got_meta[31] = sent_meta[15]
    zraw_meta[15] = zsent_meta[7]

    for g in range(ZF, ZF + ZN):
        turn(g, 0)
    for h in range(2):
        for g in range(ZN):
            zsent[h * ZN + g] = dot(zpack[...], fields[h * HALF + ZF + g]).astype(bf16)
    remote(
        zsent.at[pl.ds(other * ZN, ZN), z_rows(7)],
        zraw.at[:, z_rows(14)],
        zr_send,
        zr_recv,
        d,
        other,
    ).start()

    def send_raw(dz, _):
        for h in range(2):
            remote(
                zsent.at[pl.ds(h * ZN, ZN), z_rows(dz - 1)],
                zraw.at[:, z_rows((dz - 1) * 2 + c)],
                zr_send,
                zr_recv,
                line_chip(dz),
                h,
            ).start()
        return 0

    lax.fori_loop(1, NZ, send_raw, 0)
    zraw[:, z_rows(15), :] = zsent[pl.ds(c * ZN, ZN), z_rows(7), :]
    for k in range(1, CHUNKS):
        send_plane(k)

    most, z_most = got_meta.at[pl.ds(0, 31)], zraw_meta.at[pl.ds(0, 15)]
    pltpu.make_async_copy(most, most, me_recv).wait()
    pltpu.make_async_copy(z_most, z_most, zm_recv).wait()
    lane = iota((1, BLK), 1)
    uses = (
        (got_meta, 8, SRC_ROWS, select, (0,)),
        (zraw_meta, 4, 2 * PLANE, zselect, (0, BLK)),
    )
    for metas, per, width, matrix, offsets in uses:
        for q in range(4):
            flat = jnp.zeros((1, BLK), f32)
            for n in range(per):
                at = (lane >= n * width) & (lane < (n + 1) * width)
                flat = jnp.where(at, metas[q * per + n], flat)
            for offset in offsets:
                row, col = iota((BLK, BLK), 0) + offset, iota((BLK, BLK), 1)
                fits = (row >> 4) == ((col & (width - 1)) >> 1)
                slot = ((row & (SLOTS - 1)) + 1).astype(f32)
                matrix[offset : offset + BLK, q * BLK : (q + 1) * BLK] = one_hot(
                    fits & (flat == slot)
                )

    def from_plane(k):
        f0, fn = SPLIT[k]
        chunk = pl.ds(f0, fn)
        arrived = got.at[chunk, all_but_own]
        pltpu.make_async_copy(arrived, arrived, pl_recv.at[k]).wait()
        for g in range(f0, f0 + fn):
            total = dot(select[...], got[g])
            own[g] = total[0:SLOTS]
            part[g] = total.astype(bf16)

        def send_z(dz, _):
            remote(
                part.at[chunk, pl.ds(pl.multiple_of(dz * SLOTS, SLOTS), SLOTS)],
                zgot.at[chunk, pl.ds(pl.multiple_of((dz - 1) * SLOTS, SLOTS), SLOTS)],
                z_send.at[k],
                z_recv.at[k],
                line_chip(dz),
                c,
            ).start()
            return 0

        lax.fori_loop(1, NZ, send_z, 0)

    for k in range(CHUNKS - 2):
        from_plane(k)

    pltpu.make_async_copy(zraw.at[:, z_but_own], zraw.at[:, z_but_own], zr_recv).wait()
    for g in range(ZN):
        total = dot(zselect[...], zraw[g])
        zown[g] = total[15 * SLOTS :]
        zpart[g] = total.astype(bf16)

    def send_sums(j, _):
        rows = pl.ds(pl.multiple_of((j - 1) * SLOTS, SLOTS), SLOTS)
        remote(
            zpart.at[:, rows], zlast.at[:, rows], zp_send, zp_recv, plane_chip(j), c
        ).start()
        return 0

    lax.fori_loop(1, PLANE, send_sums, 0)

    for k in range(CHUNKS - 2, CHUNKS):
        from_plane(k)

    def from_line(k):
        f0, fn = SPLIT[k]
        chunk = pl.ds(f0, fn)
        pltpu.make_async_copy(zgot.at[chunk], zgot.at[chunk], z_recv.at[k]).wait()
        for g in range(f0, f0 + fn):
            total = own[g]
            for s in range(NZ - 1):
                total = total + zgot[g, s * SLOTS : (s + 1) * SLOTS, :].astype(f32)
            last[g * OPITCH : g * OPITCH + SLOTS, :] = total

    for k in range(CHUNKS - 1):
        from_line(k)
    pltpu.make_async_copy(zlast, zlast, zp_recv).wait()
    for g in range(ZN):
        total = zown[g]
        for s in range(PLANE - 1):
            total = total + zlast[g, s * SLOTS : (s + 1) * SLOTS, :].astype(f32)
        last[(ZF + g) * OPITCH : (ZF + g) * OPITCH + SLOTS, :] = total
    from_line(CHUNKS - 1)
    last[HALF * OPITCH :, :] = jnp.zeros((OPITCH, BLK), jnp.float32)
    for s in range(SLOTS):
        line = last[pl.ds(s, 16, stride=OPITCH), :]
        out_ref[:, s * BLK : (s + 1) * BLK] = line[0:HALF]

    for copy in upward:
        copy.wait_send()
    sideways.wait_send()

    @pl.when(corner)
    def _():
        to_relay.wait_send()

    @pl.when(jnp.logical_not(corner))
    def _():
        for copy in downward:
            copy.wait_send()

    @pl.when(relaying)
    def _():
        for copy in relayed:
            copy.wait_send()

    pltpu.make_async_copy(most, most, me_send).wait()
    pltpu.make_async_copy(z_most, z_most, zm_send).wait()
    pltpu.make_async_copy(zraw.at[:, z_but_own], zraw.at[:, z_but_own], zr_send).wait()
    pltpu.make_async_copy(zlast, zlast, zp_send).wait()
    for k in range(CHUNKS):
        chunk = pl.ds(*SPLIT[k])
        arrived = got.at[chunk, all_but_own]
        pltpu.make_async_copy(arrived, arrived, pl_send.at[k]).wait()
        pltpu.make_async_copy(zgot.at[chunk], zgot.at[chunk], z_send.at[k]).wait()


def local(ocean, grad_weight, neighbours, remap_weight, tile_src, tile_atm, atm_owner):
    bf16, f32, i32 = jnp.bfloat16, jnp.float32, jnp.int32
    vmem = pl.BlockSpec(memory_space=pltpu.VMEM)
    hbm = pl.BlockSpec(memory_space=pltpu.HBM)
    dma = pltpu.SemaphoreType.DMA
    return pl.pallas_call(
        kernel,
        out_shape=jax.ShapeDtypeStruct((HALF, NB * BLK), f32),
        in_specs=[hbm] * 7,
        out_specs=vmem,
        scratch_shapes=[
            pltpu.SMEM((4, NB), i32),
            pltpu.SMEM((1, TILES), i32),
            pltpu.VMEM((1, TILES), i32),
            pltpu.VMEM((NB, BLK), i32),
            pltpu.VMEM((2, HALF, EXT * BLK), bf16),
            pltpu.VMEM((HALF, NH * BLK), bf16),
            pltpu.VMEM((EXT, 32, BLK), bf16),
            pltpu.VMEM((NB, 4 * BLK, 2 * BLK), bf16),
            pltpu.VMEM((TILES, 3 * BLK, BLK), bf16),
            pltpu.VMEM((NB, 32, 2 * BLK), bf16),
            pltpu.VMEM((TILES * PITCH, BLK), f32),
            pltpu.VMEM((2 * HALF, TILES, BLK), bf16),
            pltpu.VMEM((PLANE * SRC_ROWS, TILES), bf16),
            pltpu.VMEM((2 * HALF, PLANE * SRC_ROWS, BLK), bf16),
            pltpu.VMEM((PLANE, 1, BLK), f32),
            pltpu.VMEM((HALF, 32 * SRC_ROWS, BLK), bf16),
            pltpu.VMEM((32, 1, BLK), f32),
            pltpu.VMEM((NZ * SLOTS, 32 * SRC_ROWS), bf16),
            pltpu.VMEM((HALF, NZ * SLOTS, BLK), bf16),
            pltpu.VMEM((HALF, SLOTS, BLK), f32),
            pltpu.VMEM((HALF, (NZ - 1) * SLOTS, BLK), bf16),
            pltpu.VMEM((16 * OPITCH, BLK), f32),
            pltpu.VMEM((PLANE * SRC_ROWS, TILES), bf16),
            pltpu.VMEM((2 * ZN, PLANE * SRC_ROWS, BLK), bf16),
            pltpu.VMEM((NZ, 1, BLK), f32),
            pltpu.VMEM((ZN, 32 * SRC_ROWS, BLK), bf16),
            pltpu.VMEM((2 * NZ, 1, BLK), f32),
            pltpu.VMEM((PLANE * SLOTS, 32 * SRC_ROWS), bf16),
            pltpu.VMEM((ZN, PLANE * SLOTS, BLK), bf16),
            pltpu.VMEM((ZN, SLOTS, BLK), f32),
            pltpu.VMEM((ZN, (PLANE - 1) * SLOTS, BLK), bf16),
            dma((6,)),
            dma,
            dma((8,)),
            dma((6,)),
            pltpu.SemaphoreType.REGULAR,
            dma,
            dma,
            dma((CHUNKS,)),
            dma((CHUNKS,)),
            dma((CHUNKS,)),
            dma((CHUNKS,)),
            dma,
            dma,
            dma,
            dma,
            dma,
            dma,
        ],
        compiler_params=pltpu.CompilerParams(
            collective_id=0, has_side_effects=True, vmem_limit_bytes=48 * 1024 * 1024
        ),
    )(
        *(
            pltpu.with_memory_space_constraint(a, pltpu.HBM)
            for a in (
                ocean,
                grad_weight.reshape(NB, 4 * BLK, 2 * BLK),
                neighbours.T,
                remap_weight,
                tile_src[None, :],
                tile_atm[None, :],
                atm_owner.reshape(NB, BLK),
            )
        )
    )


def solution(mesh):
    in_specs = (
        P("field", "dom"),
        P("dom", None, None, None),
        P("dom", None),
        P(("dom", "field"), None, None),
        P(("dom", "field")),
        P(("dom", "field")),
        P(),
    )
    out_specs = P("field", "dom")
    return jax.shard_map(local, mesh=mesh, in_specs=in_specs, out_specs=out_specs, check_vma=False)
```

```python
import functools

import jax
import jax.numpy as jnp
from jax import lax
from jax.experimental import pallas as pl
from jax.experimental.pallas import tpu as pltpu
from jax.sharding import PartitionSpec as P

MESH = pl.DeviceIdType.MESH
NX, NZ, NY = 4, 8, 4
PLANE = NX * NY
HALF = 15
BLK = 128
NB = 16
NH = 2
EXT = NB + 2 * NH
TILES = 64
SLOTS = 16
SRC_ROWS = 16
SPLIT = ((0, 4), (4, 4), (8, 2), (10, 1))
CHUNKS = len(SPLIT)
ZF, ZN = 11, 4
SENDS = (0, "meta", (0, 4), 1, 2, 3)
WAITS = (0, 1, "z", 2, 3)
Z_ORDER = (4, 3, 5, 2, 6, 1, 7)
PITCH = 40
OPITCH = 24


def coords():
    d = lax.axis_index("dom")
    return lax.div(d, NZ * NY), lax.rem(lax.div(d, NY), NZ), lax.rem(d, NY)


def chip(x, z, y):
    return (x * NZ + z) * NY + y


def kernel(
    ocean_hbm,
    gw_hbm,
    nb_hbm,
    rw_hbm,
    src_hbm,
    atm_hbm,
    owner_hbm,
    out_ref,
    nb_ref,
    src_ref,
    atm,
    owners,
    raw,
    relay,
    wide,
    gw,
    rw,
    grads,
    cont,
    fields,
    pack,
    sent,
    sent_meta,
    got,
    got_meta,
    select,
    part,
    own,
    zgot,
    last,
    zpack,
    zsent,
    zsent_meta,
    zraw,
    zraw_meta,
    zselect,
    zpart,
    zown,
    zlast,
    load_sem,
    w_sem,
    oc_send,
    oc_recv,
    near_sem,
    late_sem,
    me_send,
    me_recv,
    pl_send,
    pl_recv,
    z_send,
    z_recv,
    zm_send,
    zm_recv,
    zr_send,
    zr_recv,
    zp_send,
    zp_recv,
):
    c = lax.axis_index("field")
    d = lax.axis_index("dom")
    x, z, y = coords()
    other = 1 - c
    devices = NX * NZ * NY
    up, down = lax.rem(d + 1, devices), lax.rem(d + devices - 1, devices)

    def plane_chip(j):
        return chip(lax.rem(x + lax.div(j, NY), NX), z, lax.rem(y + lax.rem(j, NY), NY))

    def line_chip(dz):
        return chip(x, lax.rem(z + dz, NZ), y)

    ocean_in = pltpu.make_async_copy(
        ocean_hbm, raw.at[c, :, pl.ds(NH * BLK, NB * BLK)], load_sem.at[0]
    )
    ocean_in.start()
    small = [
        pltpu.make_async_copy(src, dst, load_sem.at[n])
        for n, (src, dst) in enumerate(
            ((atm_hbm, atm), (owner_hbm, owners), (nb_hbm, nb_ref), (src_hbm, src_ref)), 1
        )
    ]
    for copy in small:
        copy.start()
    gw_in = pltpu.make_async_copy(gw_hbm, gw, load_sem.at[5])
    gw_in.start()
    rw_in = pltpu.make_async_copy(rw_hbm, rw, w_sem)
    rw_in.start()

    barrier = pltpu.get_barrier_semaphore()

    def greet(dom, core, sem=barrier):
        pl.semaphore_signal(
            sem, inc=1, device_id={"dom": dom, "field": core}, device_id_type=MESH
        )

    y_ring = [chip(x, z, lax.rem(y + n, NY)) for n in range(1, NY)]
    ahead = chip(lax.rem(x + 1, NX), z, lax.rem(y + 1, NY))
    behind = chip(lax.rem(x + NX - 1, NX), z, lax.rem(y + NY - 1, NY))
    corner = (z == 0) & (y == 0)
    relaying = (z == 0) & (y == NY - 1)

    @pl.when(jnp.logical_not((z == NZ - 1) & (y == NY - 1)))
    def _():
        greet(up, 0)
        greet(up, 1)

    greet(down, 0)
    greet(down, 1)
    for n in (1, 2):
        above, under = line_chip(n), line_chip(NZ - n)
        for h in range(2):
            greet(under, h)

        @pl.when(z < NZ - n)
        def _(above=above):
            greet(above, 0)
            greet(above, 1)

    for dom in y_ring:
        greet(dom, c)
    for n in range(1, NX):
        for h in range(2):
            greet(chip(lax.rem(x + n, NX), z, y), h)

    @pl.when(z == 0)
    def _():
        greet(ahead, c)
        greet(behind, c)

    greet(d, other)

    small[0].wait()
    small[1].wait()
    bf16, f32 = jnp.bfloat16, jnp.float32

    def dot(a, b):
        return jnp.dot(a, b, preferred_element_type=f32)

    def iota(shape, dim):
        return lax.broadcasted_iota(jnp.int32, shape, dim)

    def one_hot(mask):
        return jnp.where(mask, 1.0, 0.0).astype(bf16)

    ids = atm[...]
    table = owners[...]
    halves = jnp.concatenate([table >> 4, table & 15], axis=0).astype(f32).astype(bf16)
    found = dot(halves, one_hot(iota((BLK, TILES), 0) == (ids & (BLK - 1))))
    here = iota((16, TILES), 0) == (ids >> 7)
    owner_row = jnp.sum(jnp.where(here, found[0:16], 0.0), axis=0, keepdims=True)
    slot_row = jnp.sum(jnp.where(here, found[16:32], 0.0), axis=0, keepdims=True)
    square = (TILES, TILES)
    diagonal = jnp.where(iota(square, 0) == iota(square, 1), owner_row, 0.0).astype(bf16)
    owner_col = dot(diagonal, jnp.ones(square, bf16))
    earlier = (owner_col == owner_row) & (iota(square, 0) < iota(square, 1))
    rank = jnp.sum(jnp.where(earlier, 1, 0), axis=0, keepdims=True)
    owner = owner_row.astype(jnp.int32)
    dx = ((owner >> 5) - x) & (NX - 1)
    dz = ((owner >> 2) - z) & (NZ - 1)
    dy = (owner - y) & (NY - 1)
    jj = (dx * NY + dy + PLANE - 1) & (PLANE - 1)
    z_rel = (dz + NZ - 1) & (NZ - 1)
    within = (dz * 2 + rank, jj * 2 + rank)
    plans = (
        (jj, within[0], SRC_ROWS, pack, sent_meta),
        (z_rel, within[1], 2 * PLANE, zpack, zsent_meta),
    )
    for group, inner, width, matrix, metas in plans:
        matrix[...] = one_hot(iota((PLANE * SRC_ROWS, TILES), 0) == group * width + inner)
        marked = jnp.where(iota((PLANE, TILES), 0) == group, slot_row + 1.0, 0.0).astype(bf16)
        spread = jnp.where(iota(square, 0) == iota(square, 1), inner.astype(f32), 0.0)
        inner_col = dot(spread.astype(bf16), jnp.ones((TILES, BLK), bf16))
        lanes = (iota((TILES, BLK), 1) & (width - 1)).astype(f32)
        table = dot(marked, one_hot(inner_col == lanes))
        for n in range(metas.shape[0]):
            metas[n] = table[n : n + 1]
    ocean_in.wait()

    greeted = 4 + 4 + 3 + 6 + 1 + jnp.where(z >= 1, 2, 0) + jnp.where(z >= 2, 2, 0)
    greeted = greeted + jnp.where(z == 0, 2, 0) - jnp.where(corner, 2, 0)
    pl.semaphore_wait(barrier, greeted)

    def remote(src, dst, send, recv, dom, core):
        return pltpu.make_async_remote_copy(
            src_ref=src,
            dst_ref=dst,
            send_sem=send,
            recv_sem=recv,
            device_id={"dom": dom, "field": core},
            device_id_type=MESH,
        )

    first = pl.ds(NH * BLK, NH * BLK)
    final = pl.ds(NB * BLK, NH * BLK)
    left = pl.ds(0, NH * BLK)
    right = pl.ds((NB + NH) * BLK, NH * BLK)
    middle = pl.ds(NH * BLK, NB * BLK)
    half = raw.at[c]
    upward = [
        remote(half.at[:, final], half.at[:, left], oc_send.at[n], oc_recv.at[n], up, h)
        for n, h in enumerate((c, other))
    ]
    downward = [
        remote(half.at[:, first], half.at[:, right], oc_send.at[2 + n], oc_recv.at[2 + n], down, h)
        for n, h in enumerate((c, other))
    ]
    sideways = remote(
        half.at[:, middle], half.at[:, middle], oc_send.at[4], oc_recv.at[4], d, other
    )
    to_relay = remote(half.at[:, first], relay, oc_send.at[5], oc_recv.at[5], behind, c)
    below = chip(x, NZ - 1, y)
    relayed = [
        remote(relay, half.at[:, right], oc_send.at[6 + n], oc_recv.at[2 + n], below, h)
        for n, h in enumerate((c, other))
    ]
    for copy in upward:
        copy.start()

    @pl.when(corner)
    def _():
        to_relay.start()

    @pl.when(jnp.logical_not(corner))
    def _():
        for copy in downward:
            copy.start()

    sideways.start()
    for dom in y_ring:
        greet(dom, c, near_sem)
    for n in (1, 2):

        @pl.when(z >= NZ - n)
        def _(n=n):
            greet(line_chip(n), 0, late_sem)
            greet(line_chip(n), 1, late_sem)

    @pl.when(z < 2)
    def _():
        pl.semaphore_wait(late_sem, jnp.where(z == 0, 4, 2))

    greet(line_chip(2), c, near_sem)
    greet(line_chip(NZ - 2), c, near_sem)
    @pl.when(relaying)
    def _():
        to_relay.wait_recv()
        for copy in relayed:
            copy.start()

    sideways.wait_recv()
    wide[...] = jnp.zeros_like(wide)

    def spread_blocks(blocks):
        for e in blocks:
            wide[e, 0:HALF, :] = raw[0, :, e * BLK : (e + 1) * BLK]
            wide[e, 16 : 16 + HALF, :] = raw[1, :, e * BLK : (e + 1) * BLK]

    spread_blocks(range(NH, NH + NB))
    small[2].wait()
    small[3].wait()
    rw_in.wait()
    own_block = d * NB

    def remap_values(t, _):
        s = jnp.maximum(src_ref[0, t] - own_block, 0)
        cont[pl.ds(pl.multiple_of(t * PITCH, 8), 32), :] = dot(wide[s + NH], rw[t, 0:BLK, :])
        return 0

    lax.fori_loop(0, TILES, remap_values, 0, unroll=8)
    for copy in upward + downward:
        copy.wait_recv()
    spread_blocks((0, 1, NH + NB, NH + NB + 1))

    gw_in.wait()

    first_block = d * NB - NH

    def gradient(b, _):
        picked = jnp.concatenate(
            [wide[jnp.maximum(nb_ref[k, b] - first_block, 0)] for k in range(4)], axis=1
        )
        grads[b] = jnp.dot(picked, gw[b], preferred_element_type=jnp.float32).astype(
            jnp.bfloat16
        )
        return 0

    lax.fori_loop(0, NB, gradient, 0, unroll=4)
    def remap(t, _):
        s = jnp.maximum(src_ref[0, t] - own_block, 0)
        at = pl.ds(pl.multiple_of(t * PITCH, 8), 32)
        cont[at, :] = cont[at, :] + dot(grads[s], rw[t, BLK:, :])
        return 0

    lax.fori_loop(0, TILES, remap, 0, unroll=8)

    def turn(g, _):
        for h in range(2):
            fields[h * HALF + g] = cont[pl.ds(h * 16 + g, TILES, stride=PITCH), :].astype(
                jnp.bfloat16
            )
        return 0

    pl.semaphore_wait(near_sem, 5)

    def z_rows(start):
        return pl.ds(pl.multiple_of(start * 32, 32), 32)

    own_rows = pl.ds(15 * SRC_ROWS, SRC_ROWS)
    all_but_own = pl.ds(0, 31 * SRC_ROWS)
    z_but_own = pl.ds(0, 15 * 32)
    zchunk = pl.ds(ZF, ZN)

    def send_plane(k):
        f0, fn = SPLIT[k]
        for g in range(f0, f0 + fn):
            turn(g, 0)
        for h in range(2):
            for g in range(f0, f0 + fn):
                f = h * HALF + g
                sent[f] = dot(pack[...], fields[f]).astype(bf16)
        chunk = pl.ds(f0, fn)
        remote(
            sent.at[pl.ds(other * HALF + f0, fn), own_rows],
            got.at[chunk, pl.ds(30 * SRC_ROWS, SRC_ROWS)],
            pl_send.at[k],
            pl_recv.at[k],
            d,
            other,
        ).start()

        def send(j, _):
            dom = plane_chip(j)
            for h in range(2):
                remote(
                    sent.at[
                        pl.ds(h * HALF + f0, fn),
                        pl.ds(pl.multiple_of((j - 1) * SRC_ROWS, SRC_ROWS), SRC_ROWS),
                    ],
                    got.at[
                        chunk,
                        pl.ds(pl.multiple_of(((j - 1) * 2 + c) * SRC_ROWS, SRC_ROWS), SRC_ROWS),
                    ],
                    pl_send.at[k],
                    pl_recv.at[k],
                    dom,
                    h,
                ).start()
            return 0

        lax.fori_loop(1, PLANE, send, 0)
        got[chunk, pl.ds(31 * SRC_ROWS, SRC_ROWS), :] = sent[
            pl.ds(c * HALF + f0, fn), own_rows, :
        ]

    def send_metas():
        remote(sent_meta.at[15], got_meta.at[30], me_send, me_recv, d, other).start()
        remote(zsent_meta.at[7], zraw_meta.at[14], zm_send, zm_recv, d, other).start()

        def send_meta(j, _):
            for h in range(2):
                remote(
                    sent_meta.at[j - 1],
                    got_meta.at[(j - 1) * 2 + c],
                    me_send,
                    me_recv,
                    plane_chip(j),
                    h,
                ).start()
            return 0

        def send_zmeta(dz, _):
            for h in range(2):
                remote(
                    zsent_meta.at[dz - 1],
                    zraw_meta.at[(dz - 1) * 2 + c],
                    zm_send,
                    zm_recv,
                    line_chip(dz),
                    h,
                ).start()
            return 0

        lax.fori_loop(1, PLANE, send_meta, 0)
        lax.fori_loop(1, NZ, send_zmeta, 0)
        got_meta[31] = sent_meta[15]
        zraw_meta[15] = zsent_meta[7]

    def send_z_first(g0, gn):
        for g in range(g0, g0 + gn):
            turn(ZF + g, 0)
        for h in range(2):
            for g in range(g0, g0 + gn):
                zsent[h * ZN + g] = dot(zpack[...], fields[h * HALF + ZF + g]).astype(bf16)
        remote(
            zsent.at[pl.ds(other * ZN + g0, gn), z_rows(7)],
            zraw.at[pl.ds(g0, gn), z_rows(14)],
            zr_send,
            zr_recv,
            d,
            other,
        ).start()

        def send_raw(dz, _):
            for h in range(2):
                remote(
                    zsent.at[pl.ds(h * ZN + g0, gn), pl.ds((dz - 1) * 32, 32)],
                    zraw.at[pl.ds(g0, gn), z_rows((dz - 1) * 2 + c)],
                    zr_send,
                    zr_recv,
                    line_chip(dz),
                    h,
                ).start()
            return 0

        for dz in Z_ORDER:
            send_raw(dz, 0)
        zraw[pl.ds(g0, gn), z_rows(15), :] = zsent[pl.ds(c * ZN + g0, gn), z_rows(7), :]

    for step in SENDS:
        if step == "meta":
            send_metas()
        elif isinstance(step, tuple):
            send_z_first(*step)
        else:
            send_plane(step)

    most, z_most = got_meta.at[pl.ds(0, 31)], zraw_meta.at[pl.ds(0, 15)]
    pltpu.make_async_copy(most, most, me_recv).wait()
    pltpu.make_async_copy(z_most, z_most, zm_recv).wait()
    lane = iota((1, BLK), 1)
    uses = (
        (got_meta, 8, SRC_ROWS, select, (0,)),
        (zraw_meta, 4, 2 * PLANE, zselect, (0, BLK)),
    )
    for metas, per, width, matrix, offsets in uses:
        for q in range(4):
            flat = jnp.zeros((1, BLK), f32)
            for n in range(per):
                at = (lane >= n * width) & (lane < (n + 1) * width)
                flat = jnp.where(at, metas[q * per + n], flat)
            for offset in offsets:
                row, col = iota((BLK, BLK), 0) + offset, iota((BLK, BLK), 1)
                fits = (row >> 4) == ((col & (width - 1)) >> 1)
                slot = ((row & (SLOTS - 1)) + 1).astype(f32)
                matrix[offset : offset + BLK, q * BLK : (q + 1) * BLK] = one_hot(
                    fits & (flat == slot)
                )

    def from_plane(k):
        f0, fn = SPLIT[k]
        chunk = pl.ds(f0, fn)
        arrived = got.at[chunk, all_but_own]
        pltpu.make_async_copy(arrived, arrived, pl_recv.at[k]).wait()
        for g in range(f0, f0 + fn):
            total = dot(select[...], got[g])
            own[g] = total[0:SLOTS]
            part[g] = total.astype(bf16)

        def send_z(dz, _):
            remote(
                part.at[chunk, pl.ds(dz * SLOTS, SLOTS)],
                zgot.at[chunk, pl.ds((dz - 1) * SLOTS, SLOTS)],
                z_send.at[k],
                z_recv.at[k],
                line_chip(dz),
                c,
            ).start()
            return 0

        for dz in Z_ORDER:
            send_z(dz, 0)

    def from_z_first():
        pltpu.make_async_copy(zraw.at[:, z_but_own], zraw.at[:, z_but_own], zr_recv).wait()
        for g in range(ZN):
            total = dot(zselect[...], zraw[g])
            zown[g] = total[15 * SLOTS :]
            zpart[g] = total.astype(bf16)

        def send_sums(j, _):
            rows = pl.ds(pl.multiple_of((j - 1) * SLOTS, SLOTS), SLOTS)
            remote(
                zpart.at[:, rows], zlast.at[:, rows], zp_send, zp_recv, plane_chip(j), c
            ).start()
            return 0

        lax.fori_loop(1, PLANE, send_sums, 0)

    for step in WAITS:
        if step == "z":
            from_z_first()
        else:
            from_plane(step)

    def from_line(k):
        f0, fn = SPLIT[k]
        chunk = pl.ds(f0, fn)
        pltpu.make_async_copy(zgot.at[chunk], zgot.at[chunk], z_recv.at[k]).wait()
        for g in range(f0, f0 + fn):
            total = own[g]
            for s in range(NZ - 1):
                total = total + zgot[g, s * SLOTS : (s + 1) * SLOTS, :].astype(f32)
            last[g * OPITCH : g * OPITCH + SLOTS, :] = total

    for k in range(CHUNKS - 1):
        from_line(k)
    pltpu.make_async_copy(zlast, zlast, zp_recv).wait()
    for g in range(ZN):
        total = zown[g]
        for s in range(PLANE - 1):
            total = total + zlast[g, s * SLOTS : (s + 1) * SLOTS, :].astype(f32)
        last[(ZF + g) * OPITCH : (ZF + g) * OPITCH + SLOTS, :] = total
    from_line(CHUNKS - 1)
    last[HALF * OPITCH :, :] = jnp.zeros((OPITCH, BLK), jnp.float32)
    for s in range(SLOTS):
        line = last[pl.ds(s, 16, stride=OPITCH), :]
        out_ref[:, s * BLK : (s + 1) * BLK] = line[0:HALF]

    for copy in upward:
        copy.wait_send()
    sideways.wait_send()

    @pl.when(corner)
    def _():
        to_relay.wait_send()

    @pl.when(jnp.logical_not(corner))
    def _():
        for copy in downward:
            copy.wait_send()

    @pl.when(relaying)
    def _():
        for copy in relayed:
            copy.wait_send()

    pltpu.make_async_copy(most, most, me_send).wait()
    pltpu.make_async_copy(z_most, z_most, zm_send).wait()
    pltpu.make_async_copy(zraw.at[:, z_but_own], zraw.at[:, z_but_own], zr_send).wait()
    pltpu.make_async_copy(zlast, zlast, zp_send).wait()
    for k in range(CHUNKS):
        chunk = pl.ds(*SPLIT[k])
        arrived = got.at[chunk, all_but_own]
        pltpu.make_async_copy(arrived, arrived, pl_send.at[k]).wait()
        pltpu.make_async_copy(zgot.at[chunk], zgot.at[chunk], z_send.at[k]).wait()


def local(ocean, grad_weight, neighbours, remap_weight, tile_src, tile_atm, atm_owner):
    bf16, f32, i32 = jnp.bfloat16, jnp.float32, jnp.int32
    vmem = pl.BlockSpec(memory_space=pltpu.VMEM)
    hbm = pl.BlockSpec(memory_space=pltpu.HBM)
    dma = pltpu.SemaphoreType.DMA
    return pl.pallas_call(
        kernel,
        out_shape=jax.ShapeDtypeStruct((HALF, NB * BLK), f32),
        in_specs=[hbm] * 7,
        out_specs=vmem,
        scratch_shapes=[
            pltpu.SMEM((4, NB), i32),
            pltpu.SMEM((1, TILES), i32),
            pltpu.VMEM((1, TILES), i32),
            pltpu.VMEM((NB, BLK), i32),
            pltpu.VMEM((2, HALF, EXT * BLK), bf16),
            pltpu.VMEM((HALF, NH * BLK), bf16),
            pltpu.VMEM((EXT, 32, BLK), bf16),
            pltpu.VMEM((NB, 4 * BLK, 2 * BLK), bf16),
            pltpu.VMEM((TILES, 3 * BLK, BLK), bf16),
            pltpu.VMEM((NB, 32, 2 * BLK), bf16),
            pltpu.VMEM((TILES * PITCH, BLK), f32),
            pltpu.VMEM((2 * HALF, TILES, BLK), bf16),
            pltpu.VMEM((PLANE * SRC_ROWS, TILES), bf16),
            pltpu.VMEM((2 * HALF, PLANE * SRC_ROWS, BLK), bf16),
            pltpu.VMEM((PLANE, 1, BLK), f32),
            pltpu.VMEM((HALF, 32 * SRC_ROWS, BLK), bf16),
            pltpu.VMEM((32, 1, BLK), f32),
            pltpu.VMEM((NZ * SLOTS, 32 * SRC_ROWS), bf16),
            pltpu.VMEM((HALF, NZ * SLOTS, BLK), bf16),
            pltpu.VMEM((HALF, SLOTS, BLK), f32),
            pltpu.VMEM((HALF, (NZ - 1) * SLOTS, BLK), bf16),
            pltpu.VMEM((16 * OPITCH, BLK), f32),
            pltpu.VMEM((PLANE * SRC_ROWS, TILES), bf16),
            pltpu.VMEM((2 * ZN, PLANE * SRC_ROWS, BLK), bf16),
            pltpu.VMEM((NZ, 1, BLK), f32),
            pltpu.VMEM((ZN, 32 * SRC_ROWS, BLK), bf16),
            pltpu.VMEM((2 * NZ, 1, BLK), f32),
            pltpu.VMEM((PLANE * SLOTS, 32 * SRC_ROWS), bf16),
            pltpu.VMEM((ZN, PLANE * SLOTS, BLK), bf16),
            pltpu.VMEM((ZN, SLOTS, BLK), f32),
            pltpu.VMEM((ZN, (PLANE - 1) * SLOTS, BLK), bf16),
            dma((6,)),
            dma,
            dma((8,)),
            dma((6,)),
            pltpu.SemaphoreType.REGULAR,
            pltpu.SemaphoreType.REGULAR,
            dma,
            dma,
            dma((CHUNKS,)),
            dma((CHUNKS,)),
            dma((CHUNKS,)),
            dma((CHUNKS,)),
            dma,
            dma,
            dma,
            dma,
            dma,
            dma,
        ],
        compiler_params=pltpu.CompilerParams(
            collective_id=0, has_side_effects=True, vmem_limit_bytes=48 * 1024 * 1024
        ),
    )(
        *(
            pltpu.with_memory_space_constraint(a, pltpu.HBM)
            for a in (
                ocean,
                grad_weight.reshape(NB, 4 * BLK, 2 * BLK),
                neighbours.T,
                remap_weight,
                tile_src[None, :],
                tile_atm[None, :],
                atm_owner.reshape(NB, BLK),
            )
        )
    )


def solution(mesh):
    in_specs = (
        P("field", "dom"),
        P("dom", None, None, None),
        P("dom", None),
        P(("dom", "field"), None, None),
        P(("dom", "field")),
        P(("dom", "field")),
        P(),
    )
    out_specs = P("field", "dom")
    return jax.shard_map(local, mesh=mesh, in_specs=in_specs, out_specs=out_specs, check_vma=False)
```

```python
import functools

import jax
import jax.numpy as jnp
from jax import lax
from jax.experimental import pallas as pl
from jax.experimental.pallas import tpu as pltpu
from jax.sharding import PartitionSpec as P

MESH = pl.DeviceIdType.MESH
NX, NZ, NY = 4, 8, 4
PLANE = NX * NY
HALF = 15
BLK = 128
NB = 16
NH = 2
EXT = NB + 2 * NH
TILES = 64
SLOTS = 16
SRC_ROWS = 16
SPLIT = ((0, 4), (4, 4), (8, 2), (10, 1))
CHUNKS = len(SPLIT)
ZF, ZN = 11, 4
SENDS = (0, "meta", (0, 4), 1, 2, 3)
WAITS = (0, 1, "z", 2, 3)
Z_ORDER = (4, 3, 5, 2, 6, 1, 7)
PITCH = 40
OPITCH = 24


def coords():
    d = lax.axis_index("dom")
    return lax.div(d, NZ * NY), lax.rem(lax.div(d, NY), NZ), lax.rem(d, NY)


def chip(x, z, y):
    return (x * NZ + z) * NY + y


def kernel(
    ocean_hbm,
    gw_hbm,
    nb_hbm,
    rw_hbm,
    src_hbm,
    atm_hbm,
    owner_hbm,
    out_ref,
    nb_ref,
    src_ref,
    atm,
    owners,
    raw,
    relay,
    wide,
    gw,
    rw,
    grads,
    cont,
    fields,
    pack,
    sent,
    sent_meta,
    got,
    got_meta,
    select,
    part,
    own,
    zgot,
    last,
    zpack,
    zsent,
    zsent_meta,
    zraw,
    zraw_meta,
    zselect,
    zpart,
    zown,
    zlast,
    load_sem,
    w_sem,
    oc_send,
    oc_recv,
    near_sem,
    late_sem,
    me_send,
    me_recv,
    pl_send,
    pl_recv,
    z_send,
    z_recv,
    zm_send,
    zm_recv,
    zr_send,
    zr_recv,
    zp_send,
    zp_recv,
):
    c = lax.axis_index("field")
    d = lax.axis_index("dom")
    x, z, y = coords()
    other = 1 - c
    devices = NX * NZ * NY
    up, down = lax.rem(d + 1, devices), lax.rem(d + devices - 1, devices)

    def plane_chip(j):
        return chip(lax.rem(x + lax.div(j, NY), NX), z, lax.rem(y + lax.rem(j, NY), NY))

    def line_chip(dz):
        return chip(x, lax.rem(z + dz, NZ), y)

    ocean_in = pltpu.make_async_copy(
        ocean_hbm, raw.at[c, :, pl.ds(NH * BLK, NB * BLK)], load_sem.at[0]
    )
    ocean_in.start()
    small = [
        pltpu.make_async_copy(src, dst, load_sem.at[n])
        for n, (src, dst) in enumerate(
            ((atm_hbm, atm), (owner_hbm, owners), (nb_hbm, nb_ref), (src_hbm, src_ref)), 1
        )
    ]
    for copy in small:
        copy.start()
    gw_in = pltpu.make_async_copy(gw_hbm, gw, load_sem.at[5])
    gw_in.start()
    rw_in = pltpu.make_async_copy(rw_hbm, rw, w_sem)
    rw_in.start()

    barrier = pltpu.get_barrier_semaphore()

    def greet(dom, core, sem=barrier):
        pl.semaphore_signal(
            sem, inc=1, device_id={"dom": dom, "field": core}, device_id_type=MESH
        )

    y_ring = [chip(x, z, lax.rem(y + n, NY)) for n in range(1, NY)]
    ahead = chip(lax.rem(x + 1, NX), z, lax.rem(y + 1, NY))
    behind = chip(lax.rem(x + NX - 1, NX), z, lax.rem(y + NY - 1, NY))
    corner = (z == 0) & (y == 0)
    relaying = (z == 0) & (y == NY - 1)

    @pl.when(jnp.logical_not((z == NZ - 1) & (y == NY - 1)))
    def _():
        greet(up, 0)
        greet(up, 1)

    greet(down, 0)
    greet(down, 1)
    for n in (1, 2):
        above, under = line_chip(n), line_chip(NZ - n)
        for h in range(2):
            greet(under, h)

        @pl.when(z < NZ - n)
        def _(above=above):
            greet(above, 0)
            greet(above, 1)

    for dom in y_ring:
        greet(dom, c)
    for n in range(1, NX):
        for h in range(2):
            greet(chip(lax.rem(x + n, NX), z, y), h)

    @pl.when(z == 0)
    def _():
        greet(ahead, c)
        greet(behind, c)

    greet(d, other)

    small[0].wait()
    small[1].wait()
    bf16, f32 = jnp.bfloat16, jnp.float32

    def dot(a, b):
        return jnp.dot(a, b, preferred_element_type=f32)

    def iota(shape, dim):
        return lax.broadcasted_iota(jnp.int32, shape, dim)

    def one_hot(mask):
        return jnp.where(mask, 1.0, 0.0).astype(bf16)

    ids = atm[...]
    table = owners[...]
    halves = jnp.concatenate([table >> 4, table & 15], axis=0).astype(f32).astype(bf16)
    found = dot(halves, one_hot(iota((BLK, TILES), 0) == (ids & (BLK - 1))))
    here = iota((16, TILES), 0) == (ids >> 7)
    owner_row = jnp.sum(jnp.where(here, found[0:16], 0.0), axis=0, keepdims=True)
    slot_row = jnp.sum(jnp.where(here, found[16:32], 0.0), axis=0, keepdims=True)
    square = (TILES, TILES)
    diagonal = jnp.where(iota(square, 0) == iota(square, 1), owner_row, 0.0).astype(bf16)
    owner_col = dot(diagonal, jnp.ones(square, bf16))
    earlier = (owner_col == owner_row) & (iota(square, 0) < iota(square, 1))
    rank = jnp.sum(jnp.where(earlier, 1, 0), axis=0, keepdims=True)
    owner = owner_row.astype(jnp.int32)
    dx = ((owner >> 5) - x) & (NX - 1)
    dz = ((owner >> 2) - z) & (NZ - 1)
    dy = (owner - y) & (NY - 1)
    jj = (dx * NY + dy + PLANE - 1) & (PLANE - 1)
    z_rel = (dz + NZ - 1) & (NZ - 1)
    within = (dz * 2 + rank, jj * 2 + rank)
    plans = (
        (jj, within[0], SRC_ROWS, pack, sent_meta),
        (z_rel, within[1], 2 * PLANE, zpack, zsent_meta),
    )
    for group, inner, width, matrix, metas in plans:
        matrix[...] = one_hot(iota((PLANE * SRC_ROWS, TILES), 0) == group * width + inner)
        marked = jnp.where(iota((PLANE, TILES), 0) == group, slot_row + 1.0, 0.0).astype(bf16)
        spread = jnp.where(iota(square, 0) == iota(square, 1), inner.astype(f32), 0.0)
        inner_col = dot(spread.astype(bf16), jnp.ones((TILES, BLK), bf16))
        lanes = (iota((TILES, BLK), 1) & (width - 1)).astype(f32)
        table = dot(marked, one_hot(inner_col == lanes))
        for n in range(metas.shape[0]):
            metas[n] = table[n : n + 1]
    ocean_in.wait()

    greeted = 4 + 4 + 3 + 6 + 1 + jnp.where(z >= 1, 2, 0) + jnp.where(z >= 2, 2, 0)
    greeted = greeted + jnp.where(z == 0, 2, 0) - jnp.where(corner, 2, 0)
    pl.semaphore_wait(barrier, greeted)

    def remote(src, dst, send, recv, dom, core):
        return pltpu.make_async_remote_copy(
            src_ref=src,
            dst_ref=dst,
            send_sem=send,
            recv_sem=recv,
            device_id={"dom": dom, "field": core},
            device_id_type=MESH,
        )

    first = pl.ds(NH * BLK, NH * BLK)
    final = pl.ds(NB * BLK, NH * BLK)
    left = pl.ds(0, NH * BLK)
    right = pl.ds((NB + NH) * BLK, NH * BLK)
    middle = pl.ds(NH * BLK, NB * BLK)
    half = raw.at[c]
    upward = [
        remote(half.at[:, final], half.at[:, left], oc_send.at[n], oc_recv.at[n], up, h)
        for n, h in enumerate((c, other))
    ]
    downward = [
        remote(half.at[:, first], half.at[:, right], oc_send.at[2 + n], oc_recv.at[2 + n], down, h)
        for n, h in enumerate((c, other))
    ]
    sideways = remote(
        half.at[:, middle], half.at[:, middle], oc_send.at[4], oc_recv.at[4], d, other
    )
    to_relay = remote(half.at[:, first], relay, oc_send.at[5], oc_recv.at[5], behind, c)
    below = chip(x, NZ - 1, y)
    relayed = [
        remote(relay, half.at[:, right], oc_send.at[6 + n], oc_recv.at[2 + n], below, h)
        for n, h in enumerate((c, other))
    ]
    for copy in upward:
        copy.start()

    @pl.when(corner)
    def _():
        to_relay.start()

    @pl.when(jnp.logical_not(corner))
    def _():
        for copy in downward:
            copy.start()

    sideways.start()
    for dom in y_ring:
        greet(dom, c, near_sem)
    for n in (1, 2):

        @pl.when(z >= NZ - n)
        def _(n=n):
            greet(line_chip(n), 0, late_sem)
            greet(line_chip(n), 1, late_sem)

    @pl.when(z < 2)
    def _():
        pl.semaphore_wait(late_sem, jnp.where(z == 0, 4, 2))

    greet(line_chip(2), c, near_sem)
    greet(line_chip(NZ - 2), c, near_sem)
    @pl.when(relaying)
    def _():
        to_relay.wait_recv()
        for copy in relayed:
            copy.start()

    sideways.wait_recv()
    wide[...] = jnp.zeros_like(wide)

    def spread_blocks(blocks):
        for e in blocks:
            wide[e, 0:HALF, :] = raw[0, :, e * BLK : (e + 1) * BLK]
            wide[e, 16 : 16 + HALF, :] = raw[1, :, e * BLK : (e + 1) * BLK]

    spread_blocks(range(NH, NH + NB))
    small[2].wait()
    small[3].wait()
    rw_in.wait()
    own_block = d * NB

    def remap_values(t, _):
        s = jnp.maximum(src_ref[0, t] - own_block, 0)
        cont[pl.ds(pl.multiple_of(t * PITCH, 8), 32), :] = dot(wide[s + NH], rw[t, 0:BLK, :])
        return 0

    lax.fori_loop(0, TILES, remap_values, 0, unroll=16)
    for copy in upward + downward:
        copy.wait_recv()
    spread_blocks((0, 1, NH + NB, NH + NB + 1))

    gw_in.wait()

    first_block = d * NB - NH

    def gradient(b, _):
        picked = jnp.concatenate(
            [wide[jnp.maximum(nb_ref[k, b] - first_block, 0)] for k in range(4)], axis=1
        )
        grads[b] = jnp.dot(picked, gw[b], preferred_element_type=jnp.float32).astype(
            jnp.bfloat16
        )
        return 0

    lax.fori_loop(0, NB, gradient, 0, unroll=16)
    def remap(t, _):
        s = jnp.maximum(src_ref[0, t] - own_block, 0)
        at = pl.ds(pl.multiple_of(t * PITCH, 8), 32)
        cont[at, :] = cont[at, :] + dot(grads[s], rw[t, BLK:, :])
        return 0

    lax.fori_loop(0, TILES, remap, 0, unroll=32)

    def turn(g, _):
        for h in range(2):
            fields[h * HALF + g] = cont[pl.ds(h * 16 + g, TILES, stride=PITCH), :].astype(
                jnp.bfloat16
            )
        return 0

    pl.semaphore_wait(near_sem, 5)

    def z_rows(start):
        return pl.ds(pl.multiple_of(start * 32, 32), 32)

    own_rows = pl.ds(15 * SRC_ROWS, SRC_ROWS)
    all_but_own = pl.ds(0, 31 * SRC_ROWS)
    z_but_own = pl.ds(0, 15 * 32)
    zchunk = pl.ds(ZF, ZN)

    def send_plane(k):
        f0, fn = SPLIT[k]
        for g in range(f0, f0 + fn):
            turn(g, 0)
        for h in range(2):
            for g in range(f0, f0 + fn):
                f = h * HALF + g
                sent[f] = dot(pack[...], fields[f]).astype(bf16)
        chunk = pl.ds(f0, fn)
        remote(
            sent.at[pl.ds(other * HALF + f0, fn), own_rows],
            got.at[chunk, pl.ds(30 * SRC_ROWS, SRC_ROWS)],
            pl_send.at[k],
            pl_recv.at[k],
            d,
            other,
        ).start()

        def send(j, _):
            dom = plane_chip(j)
            for h in range(2):
                remote(
                    sent.at[
                        pl.ds(h * HALF + f0, fn),
                        pl.ds(pl.multiple_of((j - 1) * SRC_ROWS, SRC_ROWS), SRC_ROWS),
                    ],
                    got.at[
                        chunk,
                        pl.ds(pl.multiple_of(((j - 1) * 2 + c) * SRC_ROWS, SRC_ROWS), SRC_ROWS),
                    ],
                    pl_send.at[k],
                    pl_recv.at[k],
                    dom,
                    h,
                ).start()
            return 0

        lax.fori_loop(1, PLANE, send, 0)
        got[chunk, pl.ds(31 * SRC_ROWS, SRC_ROWS), :] = sent[
            pl.ds(c * HALF + f0, fn), own_rows, :
        ]

    def send_metas():
        remote(sent_meta.at[15], got_meta.at[30], me_send, me_recv, d, other).start()
        remote(zsent_meta.at[7], zraw_meta.at[14], zm_send, zm_recv, d, other).start()

        def send_meta(j, _):
            for h in range(2):
                remote(
                    sent_meta.at[j - 1],
                    got_meta.at[(j - 1) * 2 + c],
                    me_send,
                    me_recv,
                    plane_chip(j),
                    h,
                ).start()
            return 0

        def send_zmeta(dz, _):
            for h in range(2):
                remote(
                    zsent_meta.at[dz - 1],
                    zraw_meta.at[(dz - 1) * 2 + c],
                    zm_send,
                    zm_recv,
                    line_chip(dz),
                    h,
                ).start()
            return 0

        lax.fori_loop(1, PLANE, send_meta, 0)
        lax.fori_loop(1, NZ, send_zmeta, 0)
        got_meta[31] = sent_meta[15]
        zraw_meta[15] = zsent_meta[7]

    def send_z_first(g0, gn):
        for g in range(g0, g0 + gn):
            turn(ZF + g, 0)
        for h in range(2):
            for g in range(g0, g0 + gn):
                zsent[h * ZN + g] = dot(zpack[...], fields[h * HALF + ZF + g]).astype(bf16)
        remote(
            zsent.at[pl.ds(other * ZN + g0, gn), z_rows(7)],
            zraw.at[pl.ds(g0, gn), z_rows(14)],
            zr_send,
            zr_recv,
            d,
            other,
        ).start()

        def send_raw(dz, _):
            for h in range(2):
                remote(
                    zsent.at[pl.ds(h * ZN + g0, gn), pl.ds((dz - 1) * 32, 32)],
                    zraw.at[pl.ds(g0, gn), z_rows((dz - 1) * 2 + c)],
                    zr_send,
                    zr_recv,
                    line_chip(dz),
                    h,
                ).start()
            return 0

        for dz in Z_ORDER:
            send_raw(dz, 0)
        zraw[pl.ds(g0, gn), z_rows(15), :] = zsent[pl.ds(c * ZN + g0, gn), z_rows(7), :]

    for step in SENDS:
        if step == "meta":
            send_metas()
        elif isinstance(step, tuple):
            send_z_first(*step)
        else:
            send_plane(step)

    most, z_most = got_meta.at[pl.ds(0, 31)], zraw_meta.at[pl.ds(0, 15)]
    pltpu.make_async_copy(most, most, me_recv).wait()
    pltpu.make_async_copy(z_most, z_most, zm_recv).wait()
    lane = iota((1, BLK), 1)
    uses = (
        (got_meta, 8, SRC_ROWS, select, (0,)),
        (zraw_meta, 4, 2 * PLANE, zselect, (0, BLK)),
    )
    for metas, per, width, matrix, offsets in uses:
        for q in range(4):
            flat = jnp.zeros((1, BLK), f32)
            for n in range(per):
                at = (lane >= n * width) & (lane < (n + 1) * width)
                flat = jnp.where(at, metas[q * per + n], flat)
            for offset in offsets:
                row, col = iota((BLK, BLK), 0) + offset, iota((BLK, BLK), 1)
                fits = (row >> 4) == ((col & (width - 1)) >> 1)
                slot = ((row & (SLOTS - 1)) + 1).astype(f32)
                matrix[offset : offset + BLK, q * BLK : (q + 1) * BLK] = one_hot(
                    fits & (flat == slot)
                )

    def from_plane(k):
        f0, fn = SPLIT[k]
        chunk = pl.ds(f0, fn)
        arrived = got.at[chunk, all_but_own]
        pltpu.make_async_copy(arrived, arrived, pl_recv.at[k]).wait()
        for g in range(f0, f0 + fn):
            total = dot(select[...], got[g])
            own[g] = total[0:SLOTS]
            part[g] = total.astype(bf16)

        def send_z(dz, _):
            remote(
                part.at[chunk, pl.ds(dz * SLOTS, SLOTS)],
                zgot.at[chunk, pl.ds((dz - 1) * SLOTS, SLOTS)],
                z_send.at[k],
                z_recv.at[k],
                line_chip(dz),
                c,
            ).start()
            return 0

        for dz in Z_ORDER:
            send_z(dz, 0)

    def from_z_first():
        pltpu.make_async_copy(zraw.at[:, z_but_own], zraw.at[:, z_but_own], zr_recv).wait()
        for g in range(ZN):
            total = dot(zselect[...], zraw[g])
            zown[g] = total[15 * SLOTS :]
            zpart[g] = total.astype(bf16)

        def send_sums(j, _):
            rows = pl.ds(pl.multiple_of((j - 1) * SLOTS, SLOTS), SLOTS)
            remote(
                zpart.at[:, rows], zlast.at[:, rows], zp_send, zp_recv, plane_chip(j), c
            ).start()
            return 0

        lax.fori_loop(1, PLANE, send_sums, 0)

    for step in WAITS:
        if step == "z":
            from_z_first()
        else:
            from_plane(step)

    def from_line(k):
        f0, fn = SPLIT[k]
        chunk = pl.ds(f0, fn)
        pltpu.make_async_copy(zgot.at[chunk], zgot.at[chunk], z_recv.at[k]).wait()
        for g in range(f0, f0 + fn):
            total = own[g]
            for s in range(NZ - 1):
                total = total + zgot[g, s * SLOTS : (s + 1) * SLOTS, :].astype(f32)
            last[g * OPITCH : g * OPITCH + SLOTS, :] = total

    for k in range(CHUNKS - 1):
        from_line(k)
    pltpu.make_async_copy(zlast, zlast, zp_recv).wait()
    for g in range(ZN):
        total = zown[g]
        for s in range(PLANE - 1):
            total = total + zlast[g, s * SLOTS : (s + 1) * SLOTS, :].astype(f32)
        last[(ZF + g) * OPITCH : (ZF + g) * OPITCH + SLOTS, :] = total
    from_line(CHUNKS - 1)
    last[HALF * OPITCH :, :] = jnp.zeros((OPITCH, BLK), jnp.float32)
    for s in range(SLOTS):
        line = last[pl.ds(s, 16, stride=OPITCH), :]
        out_ref[:, s * BLK : (s + 1) * BLK] = line[0:HALF]

    for copy in upward:
        copy.wait_send()
    sideways.wait_send()

    @pl.when(corner)
    def _():
        to_relay.wait_send()

    @pl.when(jnp.logical_not(corner))
    def _():
        for copy in downward:
            copy.wait_send()

    @pl.when(relaying)
    def _():
        for copy in relayed:
            copy.wait_send()

    pltpu.make_async_copy(most, most, me_send).wait()
    pltpu.make_async_copy(z_most, z_most, zm_send).wait()
    pltpu.make_async_copy(zraw.at[:, z_but_own], zraw.at[:, z_but_own], zr_send).wait()
    pltpu.make_async_copy(zlast, zlast, zp_send).wait()
    for k in range(CHUNKS):
        chunk = pl.ds(*SPLIT[k])
        arrived = got.at[chunk, all_but_own]
        pltpu.make_async_copy(arrived, arrived, pl_send.at[k]).wait()
        pltpu.make_async_copy(zgot.at[chunk], zgot.at[chunk], z_send.at[k]).wait()


def local(ocean, grad_weight, neighbours, remap_weight, tile_src, tile_atm, atm_owner):
    bf16, f32, i32 = jnp.bfloat16, jnp.float32, jnp.int32
    vmem = pl.BlockSpec(memory_space=pltpu.VMEM)
    hbm = pl.BlockSpec(memory_space=pltpu.HBM)
    dma = pltpu.SemaphoreType.DMA
    return pl.pallas_call(
        kernel,
        out_shape=jax.ShapeDtypeStruct((HALF, NB * BLK), f32),
        in_specs=[hbm] * 7,
        out_specs=vmem,
        scratch_shapes=[
            pltpu.SMEM((4, NB), i32),
            pltpu.SMEM((1, TILES), i32),
            pltpu.VMEM((1, TILES), i32),
            pltpu.VMEM((NB, BLK), i32),
            pltpu.VMEM((2, HALF, EXT * BLK), bf16),
            pltpu.VMEM((HALF, NH * BLK), bf16),
            pltpu.VMEM((EXT, 32, BLK), bf16),
            pltpu.VMEM((NB, 4 * BLK, 2 * BLK), bf16),
            pltpu.VMEM((TILES, 3 * BLK, BLK), bf16),
            pltpu.VMEM((NB, 32, 2 * BLK), bf16),
            pltpu.VMEM((TILES * PITCH, BLK), f32),
            pltpu.VMEM((2 * HALF, TILES, BLK), bf16),
            pltpu.VMEM((PLANE * SRC_ROWS, TILES), bf16),
            pltpu.VMEM((2 * HALF, PLANE * SRC_ROWS, BLK), bf16),
            pltpu.VMEM((PLANE, 1, BLK), f32),
            pltpu.VMEM((HALF, 32 * SRC_ROWS, BLK), bf16),
            pltpu.VMEM((32, 1, BLK), f32),
            pltpu.VMEM((NZ * SLOTS, 32 * SRC_ROWS), bf16),
            pltpu.VMEM((HALF, NZ * SLOTS, BLK), bf16),
            pltpu.VMEM((HALF, SLOTS, BLK), f32),
            pltpu.VMEM((HALF, (NZ - 1) * SLOTS, BLK), bf16),
            pltpu.VMEM((16 * OPITCH, BLK), f32),
            pltpu.VMEM((PLANE * SRC_ROWS, TILES), bf16),
            pltpu.VMEM((2 * ZN, PLANE * SRC_ROWS, BLK), bf16),
            pltpu.VMEM((NZ, 1, BLK), f32),
            pltpu.VMEM((ZN, 32 * SRC_ROWS, BLK), bf16),
            pltpu.VMEM((2 * NZ, 1, BLK), f32),
            pltpu.VMEM((PLANE * SLOTS, 32 * SRC_ROWS), bf16),
            pltpu.VMEM((ZN, PLANE * SLOTS, BLK), bf16),
            pltpu.VMEM((ZN, SLOTS, BLK), f32),
            pltpu.VMEM((ZN, (PLANE - 1) * SLOTS, BLK), bf16),
            dma((6,)),
            dma,
            dma((8,)),
            dma((6,)),
            pltpu.SemaphoreType.REGULAR,
            pltpu.SemaphoreType.REGULAR,
            dma,
            dma,
            dma((CHUNKS,)),
            dma((CHUNKS,)),
            dma((CHUNKS,)),
            dma((CHUNKS,)),
            dma,
            dma,
            dma,
            dma,
            dma,
            dma,
        ],
        compiler_params=pltpu.CompilerParams(
            collective_id=0, has_side_effects=True, vmem_limit_bytes=48 * 1024 * 1024
        ),
    )(
        *(
            pltpu.with_memory_space_constraint(a, pltpu.HBM)
            for a in (
                ocean,
                grad_weight.reshape(NB, 4 * BLK, 2 * BLK),
                neighbours.T,
                remap_weight,
                tile_src[None, :],
                tile_atm[None, :],
                atm_owner.reshape(NB, BLK),
            )
        )
    )


def solution(mesh):
    in_specs = (
        P("field", "dom"),
        P("dom", None, None, None),
        P("dom", None),
        P(("dom", "field"), None, None),
        P(("dom", "field")),
        P(("dom", "field")),
        P(),
    )
    out_specs = P("field", "dom")
    return jax.shard_map(local, mesh=mesh, in_specs=in_specs, out_specs=out_specs, check_vma=False)
```

```python
import functools

import jax
import jax.numpy as jnp
from jax import lax
from jax.experimental import pallas as pl
from jax.experimental.pallas import tpu as pltpu
from jax.sharding import PartitionSpec as P

MESH = pl.DeviceIdType.MESH
NX, NZ, NY = 4, 8, 4
PLANE = NX * NY
HALF = 15
BLK = 128
NB = 16
NH = 2
EXT = NB + 2 * NH
TILES = 64
SLOTS = 16
SRC_ROWS = 16
SPLIT = ((0, 4), (4, 4), (8, 2), (10, 1))
CHUNKS = len(SPLIT)
ZF, ZN = 11, 4
SENDS = (0, "meta", (0, 4), 1, 2, 3)
WAITS = (0, 1, "z", 2, 3)
Z_ORDER = (4, 3, 5, 2, 6, 1, 7)
PITCH = 40
OPITCH = 24


def coords():
    d = lax.axis_index("dom")
    return lax.div(d, NZ * NY), lax.rem(lax.div(d, NY), NZ), lax.rem(d, NY)


def chip(x, z, y):
    return (x * NZ + z) * NY + y


def kernel(
    ocean_hbm,
    gw_hbm,
    nb_hbm,
    rw_hbm,
    src_hbm,
    atm_hbm,
    owner_hbm,
    out_ref,
    nb_ref,
    src_ref,
    atm,
    owners,
    raw,
    relay,
    wide,
    gw,
    rw,
    grads,
    cont,
    fields,
    pack,
    sent,
    sent_meta,
    got,
    got_meta,
    select,
    part,
    own,
    zgot,
    last,
    zpack,
    zsent,
    zsent_meta,
    zraw,
    zraw_meta,
    zselect,
    zpart,
    zown,
    zlast,
    load_sem,
    w_sem,
    oc_send,
    oc_recv,
    near_sem,
    late_sem,
    me_send,
    me_recv,
    pl_send,
    pl_recv,
    z_send,
    z_recv,
    zm_send,
    zm_recv,
    zr_send,
    zr_recv,
    zp_send,
    zp_recv,
):
    c = lax.axis_index("field")
    d = lax.axis_index("dom")
    x, z, y = coords()
    other = 1 - c
    devices = NX * NZ * NY
    up, down = lax.rem(d + 1, devices), lax.rem(d + devices - 1, devices)

    def plane_chip(j):
        return chip(lax.rem(x + lax.div(j, NY), NX), z, lax.rem(y + lax.rem(j, NY), NY))

    def line_chip(dz):
        return chip(x, lax.rem(z + dz, NZ), y)

    ocean_in = pltpu.make_async_copy(
        ocean_hbm, raw.at[c, :, pl.ds(NH * BLK, NB * BLK)], load_sem.at[0]
    )
    ocean_in.start()
    small = [
        pltpu.make_async_copy(src, dst, load_sem.at[n])
        for n, (src, dst) in enumerate(
            ((atm_hbm, atm), (owner_hbm, owners), (nb_hbm, nb_ref), (src_hbm, src_ref)), 1
        )
    ]
    for copy in small:
        copy.start()
    gw_in = pltpu.make_async_copy(gw_hbm, gw, load_sem.at[5])
    gw_in.start()
    rw_in = pltpu.make_async_copy(rw_hbm, rw, w_sem)
    rw_in.start()

    barrier = pltpu.get_barrier_semaphore()

    def greet(dom, core, sem=barrier):
        pl.semaphore_signal(
            sem, inc=1, device_id={"dom": dom, "field": core}, device_id_type=MESH
        )

    y_ring = [chip(x, z, lax.rem(y + n, NY)) for n in range(1, NY)]
    ahead = chip(lax.rem(x + 1, NX), z, lax.rem(y + 1, NY))
    behind = chip(lax.rem(x + NX - 1, NX), z, lax.rem(y + NY - 1, NY))
    corner = (z == 0) & (y == 0)
    relaying = (z == 0) & (y == NY - 1)

    @pl.when(jnp.logical_not((z == NZ - 1) & (y == NY - 1)))
    def _():
        greet(up, 0)
        greet(up, 1)

    greet(down, 0)
    greet(down, 1)
    for n in (1, 2):
        above, under = line_chip(n), line_chip(NZ - n)
        for h in range(2):
            greet(under, h)

        @pl.when(z < NZ - n)
        def _(above=above):
            greet(above, 0)
            greet(above, 1)

    for dom in y_ring:
        greet(dom, c)
    for n in range(1, NX):
        for h in range(2):
            greet(chip(lax.rem(x + n, NX), z, y), h)

    @pl.when(z == 0)
    def _():
        greet(ahead, c)
        greet(behind, c)

    greet(d, other)

    small[0].wait()
    small[1].wait()
    bf16, f32 = jnp.bfloat16, jnp.float32

    def dot(a, b):
        return jnp.dot(a, b, preferred_element_type=f32)

    def iota(shape, dim):
        return lax.broadcasted_iota(jnp.int32, shape, dim)

    def one_hot(mask):
        return jnp.where(mask, 1.0, 0.0).astype(bf16)

    ids = atm[...]
    table = owners[...]
    halves = jnp.concatenate([table >> 4, table & 15], axis=0).astype(f32).astype(bf16)
    found = dot(halves, one_hot(iota((BLK, TILES), 0) == (ids & (BLK - 1))))
    here = iota((16, TILES), 0) == (ids >> 7)
    owner_row = jnp.sum(jnp.where(here, found[0:16], 0.0), axis=0, keepdims=True)
    slot_row = jnp.sum(jnp.where(here, found[16:32], 0.0), axis=0, keepdims=True)
    square = (TILES, TILES)
    diagonal = jnp.where(iota(square, 0) == iota(square, 1), owner_row, 0.0).astype(bf16)
    owner_col = dot(diagonal, jnp.ones(square, bf16))
    earlier = (owner_col == owner_row) & (iota(square, 0) < iota(square, 1))
    rank = jnp.sum(jnp.where(earlier, 1, 0), axis=0, keepdims=True)
    owner = owner_row.astype(jnp.int32)
    dx = ((owner >> 5) - x) & (NX - 1)
    dz = ((owner >> 2) - z) & (NZ - 1)
    dy = (owner - y) & (NY - 1)
    jj = (dx * NY + dy + PLANE - 1) & (PLANE - 1)
    z_rel = (dz + NZ - 1) & (NZ - 1)
    within = (dz * 2 + rank, jj * 2 + rank)
    plans = (
        (jj, within[0], SRC_ROWS, pack, sent_meta),
        (z_rel, within[1], 2 * PLANE, zpack, zsent_meta),
    )
    for group, inner, width, matrix, metas in plans:
        matrix[...] = one_hot(iota((PLANE * SRC_ROWS, TILES), 0) == group * width + inner)
        marked = jnp.where(iota((PLANE, TILES), 0) == group, slot_row + 1.0, 0.0).astype(bf16)
        spread = jnp.where(iota(square, 0) == iota(square, 1), inner.astype(f32), 0.0)
        inner_col = dot(spread.astype(bf16), jnp.ones((TILES, BLK), bf16))
        lanes = (iota((TILES, BLK), 1) & (width - 1)).astype(f32)
        table = dot(marked, one_hot(inner_col == lanes))
        for n in range(metas.shape[0]):
            metas[n] = table[n : n + 1]
    ocean_in.wait()

    greeted = 4 + 4 + 3 + 6 + 1 + jnp.where(z >= 1, 2, 0) + jnp.where(z >= 2, 2, 0)
    greeted = greeted + jnp.where(z == 0, 2, 0) - jnp.where(corner, 2, 0)
    pl.semaphore_wait(barrier, greeted)

    def remote(src, dst, send, recv, dom, core):
        return pltpu.make_async_remote_copy(
            src_ref=src,
            dst_ref=dst,
            send_sem=send,
            recv_sem=recv,
            device_id={"dom": dom, "field": core},
            device_id_type=MESH,
        )

    first = pl.ds(NH * BLK, NH * BLK)
    final = pl.ds(NB * BLK, NH * BLK)
    left = pl.ds(0, NH * BLK)
    right = pl.ds((NB + NH) * BLK, NH * BLK)
    middle = pl.ds(NH * BLK, NB * BLK)
    half = raw.at[c]
    upward = [
        remote(half.at[:, final], half.at[:, left], oc_send.at[n], oc_recv.at[n], up, h)
        for n, h in enumerate((c, other))
    ]
    downward = [
        remote(half.at[:, first], half.at[:, right], oc_send.at[2 + n], oc_recv.at[2 + n], down, h)
        for n, h in enumerate((c, other))
    ]
    sideways = remote(
        half.at[:, middle], half.at[:, middle], oc_send.at[4], oc_recv.at[4], d, other
    )
    to_relay = remote(half.at[:, first], relay, oc_send.at[5], oc_recv.at[5], behind, c)
    below = chip(x, NZ - 1, y)
    relayed = [
        remote(relay, half.at[:, right], oc_send.at[6 + n], oc_recv.at[2 + n], below, h)
        for n, h in enumerate((c, other))
    ]
    for copy in upward:
        copy.start()

    @pl.when(corner)
    def _():
        to_relay.start()

    @pl.when(jnp.logical_not(corner))
    def _():
        for copy in downward:
            copy.start()

    sideways.start()
    for dom in y_ring:
        greet(dom, c, near_sem)
    for n in (1, 2):

        @pl.when(z >= NZ - n)
        def _(n=n):
            greet(line_chip(n), 0, late_sem)
            greet(line_chip(n), 1, late_sem)

    @pl.when(z < 2)
    def _():
        pl.semaphore_wait(late_sem, jnp.where(z == 0, 4, 2))

    greet(line_chip(2), c, near_sem)
    greet(line_chip(NZ - 2), c, near_sem)
    @pl.when(relaying)
    def _():
        to_relay.wait_recv()
        for copy in relayed:
            copy.start()

    sideways.wait_recv()
    wide[...] = jnp.zeros_like(wide)

    def spread_blocks(blocks):
        for e in blocks:
            wide[e, 0:HALF, :] = raw[0, :, e * BLK : (e + 1) * BLK]
            wide[e, 16 : 16 + HALF, :] = raw[1, :, e * BLK : (e + 1) * BLK]

    spread_blocks(range(NH, NH + NB))
    small[2].wait()
    small[3].wait()
    rw_in.wait()
    own_block = d * NB

    def remap_values(t, _):
        s = jnp.maximum(src_ref[0, t] - own_block, 0)
        cont[pl.ds(pl.multiple_of(t * PITCH, 8), 32), :] = dot(wide[s + NH], rw[t, 0:BLK, :])
        return 0

    lax.fori_loop(0, TILES, remap_values, 0, unroll=16)
    for copy in upward + downward:
        copy.wait_recv()
    spread_blocks((0, 1, NH + NB, NH + NB + 1))

    gw_in.wait()

    first_block = d * NB - NH

    def gradient(b, _):
        picked = jnp.concatenate(
            [wide[jnp.maximum(nb_ref[k, b] - first_block, 0)] for k in range(4)], axis=1
        )
        grads[b] = jnp.dot(picked, gw[b], preferred_element_type=jnp.float32).astype(
            jnp.bfloat16
        )
        return 0

    lax.fori_loop(0, NB, gradient, 0, unroll=16)
    def remap(t, _):
        s = jnp.maximum(src_ref[0, t] - own_block, 0)
        at = pl.ds(pl.multiple_of(t * PITCH, 8), 32)
        cont[at, :] = cont[at, :] + dot(grads[s], rw[t, BLK:, :])
        return 0

    lax.fori_loop(0, TILES, remap, 0, unroll=32)

    def turn(g, _):
        for h in range(2):
            fields[h * HALF + g] = cont[pl.ds(h * 16 + g, TILES, stride=PITCH), :].astype(
                jnp.bfloat16
            )
        return 0

    pl.semaphore_wait(near_sem, 5)

    def z_rows(start):
        return pl.ds(pl.multiple_of(start * 32, 32), 32)

    own_rows = pl.ds(15 * SRC_ROWS, SRC_ROWS)
    all_but_own = pl.ds(0, 31 * SRC_ROWS)
    z_but_own = pl.ds(0, 15 * 32)
    zchunk = pl.ds(ZF, ZN)

    def send_plane(k):
        f0, fn = SPLIT[k]
        for g in range(f0, f0 + fn):
            turn(g, 0)
        for h in range(2):
            for g in range(f0, f0 + fn, 2):
                f, n = h * HALF + g, min(2, f0 + fn - g)
                pair = jnp.concatenate([fields[f + i] for i in range(n)], axis=1)
                packed = dot(pack[...], pair).astype(bf16)
                for i in range(n):
                    sent[f + i] = packed[:, i * BLK : (i + 1) * BLK]
        chunk = pl.ds(f0, fn)
        remote(
            sent.at[pl.ds(other * HALF + f0, fn), own_rows],
            got.at[chunk, pl.ds(30 * SRC_ROWS, SRC_ROWS)],
            pl_send.at[k],
            pl_recv.at[k],
            d,
            other,
        ).start()

        def send(j, _):
            dom = plane_chip(j)
            for h in range(2):
                remote(
                    sent.at[
                        pl.ds(h * HALF + f0, fn),
                        pl.ds(pl.multiple_of((j - 1) * SRC_ROWS, SRC_ROWS), SRC_ROWS),
                    ],
                    got.at[
                        chunk,
                        pl.ds(pl.multiple_of(((j - 1) * 2 + c) * SRC_ROWS, SRC_ROWS), SRC_ROWS),
                    ],
                    pl_send.at[k],
                    pl_recv.at[k],
                    dom,
                    h,
                ).start()
            return 0

        lax.fori_loop(1, PLANE, send, 0)
        got[chunk, pl.ds(31 * SRC_ROWS, SRC_ROWS), :] = sent[
            pl.ds(c * HALF + f0, fn), own_rows, :
        ]

    def send_metas():
        remote(sent_meta.at[15], got_meta.at[30], me_send, me_recv, d, other).start()
        remote(zsent_meta.at[7], zraw_meta.at[14], zm_send, zm_recv, d, other).start()

        def send_meta(j, _):
            for h in range(2):
                remote(
                    sent_meta.at[j - 1],
                    got_meta.at[(j - 1) * 2 + c],
                    me_send,
                    me_recv,
                    plane_chip(j),
                    h,
                ).start()
            return 0

        def send_zmeta(dz, _):
            for h in range(2):
                remote(
                    zsent_meta.at[dz - 1],
                    zraw_meta.at[(dz - 1) * 2 + c],
                    zm_send,
                    zm_recv,
                    line_chip(dz),
                    h,
                ).start()
            return 0

        lax.fori_loop(1, PLANE, send_meta, 0)
        lax.fori_loop(1, NZ, send_zmeta, 0)
        got_meta[31] = sent_meta[15]
        zraw_meta[15] = zsent_meta[7]

    def send_z_first(g0, gn):
        for g in range(g0, g0 + gn):
            turn(ZF + g, 0)
        for h in range(2):
            for g in range(g0, g0 + gn):
                zsent[h * ZN + g] = dot(zpack[...], fields[h * HALF + ZF + g]).astype(bf16)
        remote(
            zsent.at[pl.ds(other * ZN + g0, gn), z_rows(7)],
            zraw.at[pl.ds(g0, gn), z_rows(14)],
            zr_send,
            zr_recv,
            d,
            other,
        ).start()

        def send_raw(dz, _):
            for h in range(2):
                remote(
                    zsent.at[pl.ds(h * ZN + g0, gn), pl.ds((dz - 1) * 32, 32)],
                    zraw.at[pl.ds(g0, gn), z_rows((dz - 1) * 2 + c)],
                    zr_send,
                    zr_recv,
                    line_chip(dz),
                    h,
                ).start()
            return 0

        for dz in Z_ORDER:
            send_raw(dz, 0)
        zraw[pl.ds(g0, gn), z_rows(15), :] = zsent[pl.ds(c * ZN + g0, gn), z_rows(7), :]

    for step in SENDS:
        if step == "meta":
            send_metas()
        elif isinstance(step, tuple):
            send_z_first(*step)
        else:
            send_plane(step)

    most, z_most = got_meta.at[pl.ds(0, 31)], zraw_meta.at[pl.ds(0, 15)]
    pltpu.make_async_copy(most, most, me_recv).wait()
    pltpu.make_async_copy(z_most, z_most, zm_recv).wait()
    lane = iota((1, BLK), 1)
    uses = (
        (got_meta, 8, SRC_ROWS, select, (0,)),
        (zraw_meta, 4, 2 * PLANE, zselect, (0, BLK)),
    )
    for metas, per, width, matrix, offsets in uses:
        for q in range(4):
            flat = jnp.zeros((1, BLK), f32)
            for n in range(per):
                at = (lane >= n * width) & (lane < (n + 1) * width)
                flat = jnp.where(at, metas[q * per + n], flat)
            for offset in offsets:
                row, col = iota((BLK, BLK), 0) + offset, iota((BLK, BLK), 1)
                fits = (row >> 4) == ((col & (width - 1)) >> 1)
                slot = ((row & (SLOTS - 1)) + 1).astype(f32)
                matrix[offset : offset + BLK, q * BLK : (q + 1) * BLK] = one_hot(
                    fits & (flat == slot)
                )

    def from_plane(k):
        f0, fn = SPLIT[k]
        chunk = pl.ds(f0, fn)
        arrived = got.at[chunk, all_but_own]
        pltpu.make_async_copy(arrived, arrived, pl_recv.at[k]).wait()
        for g in range(f0, f0 + fn, 2):
            n = min(2, f0 + fn - g)
            pair = jnp.concatenate([got[g + i] for i in range(n)], axis=1)
            totals = dot(select[...], pair)
            for i in range(n):
                total = totals[:, i * BLK : (i + 1) * BLK]
                own[g + i] = total[0:SLOTS]
                part[g + i] = total.astype(bf16)

        def send_z(dz, _):
            remote(
                part.at[chunk, pl.ds(dz * SLOTS, SLOTS)],
                zgot.at[chunk, pl.ds((dz - 1) * SLOTS, SLOTS)],
                z_send.at[k],
                z_recv.at[k],
                line_chip(dz),
                c,
            ).start()
            return 0

        for dz in Z_ORDER:
            send_z(dz, 0)

    def from_z_first():
        pltpu.make_async_copy(zraw.at[:, z_but_own], zraw.at[:, z_but_own], zr_recv).wait()
        for g in range(ZN):
            total = dot(zselect[...], zraw[g])
            zown[g] = total[15 * SLOTS :]
            zpart[g] = total.astype(bf16)

        def send_sums(j, _):
            rows = pl.ds(pl.multiple_of((j - 1) * SLOTS, SLOTS), SLOTS)
            remote(
                zpart.at[:, rows], zlast.at[:, rows], zp_send, zp_recv, plane_chip(j), c
            ).start()
            return 0

        lax.fori_loop(1, PLANE, send_sums, 0)

    for step in WAITS:
        if step == "z":
            from_z_first()
        else:
            from_plane(step)

    def from_line(k):
        f0, fn = SPLIT[k]
        chunk = pl.ds(f0, fn)
        pltpu.make_async_copy(zgot.at[chunk], zgot.at[chunk], z_recv.at[k]).wait()
        for g in range(f0, f0 + fn):
            total = own[g]
            for s in range(NZ - 1):
                total = total + zgot[g, s * SLOTS : (s + 1) * SLOTS, :].astype(f32)
            last[g * OPITCH : g * OPITCH + SLOTS, :] = total

    for k in range(CHUNKS - 1):
        from_line(k)
    pltpu.make_async_copy(zlast, zlast, zp_recv).wait()
    for g in range(ZN):
        total = zown[g]
        for s in range(PLANE - 1):
            total = total + zlast[g, s * SLOTS : (s + 1) * SLOTS, :].astype(f32)
        last[(ZF + g) * OPITCH : (ZF + g) * OPITCH + SLOTS, :] = total
    from_line(CHUNKS - 1)
    last[HALF * OPITCH :, :] = jnp.zeros((OPITCH, BLK), jnp.float32)
    for s in range(SLOTS):
        line = last[pl.ds(s, 16, stride=OPITCH), :]
        out_ref[:, s * BLK : (s + 1) * BLK] = line[0:HALF]

    for copy in upward:
        copy.wait_send()
    sideways.wait_send()

    @pl.when(corner)
    def _():
        to_relay.wait_send()

    @pl.when(jnp.logical_not(corner))
    def _():
        for copy in downward:
            copy.wait_send()

    @pl.when(relaying)
    def _():
        for copy in relayed:
            copy.wait_send()

    pltpu.make_async_copy(most, most, me_send).wait()
    pltpu.make_async_copy(z_most, z_most, zm_send).wait()
    pltpu.make_async_copy(zraw.at[:, z_but_own], zraw.at[:, z_but_own], zr_send).wait()
    pltpu.make_async_copy(zlast, zlast, zp_send).wait()
    for k in range(CHUNKS):
        chunk = pl.ds(*SPLIT[k])
        arrived = got.at[chunk, all_but_own]
        pltpu.make_async_copy(arrived, arrived, pl_send.at[k]).wait()
        pltpu.make_async_copy(zgot.at[chunk], zgot.at[chunk], z_send.at[k]).wait()


def local(ocean, grad_weight, neighbours, remap_weight, tile_src, tile_atm, atm_owner):
    bf16, f32, i32 = jnp.bfloat16, jnp.float32, jnp.int32
    vmem = pl.BlockSpec(memory_space=pltpu.VMEM)
    hbm = pl.BlockSpec(memory_space=pltpu.HBM)
    dma = pltpu.SemaphoreType.DMA
    return pl.pallas_call(
        kernel,
        out_shape=jax.ShapeDtypeStruct((HALF, NB * BLK), f32),
        in_specs=[hbm] * 7,
        out_specs=vmem,
        scratch_shapes=[
            pltpu.SMEM((4, NB), i32),
            pltpu.SMEM((1, TILES), i32),
            pltpu.VMEM((1, TILES), i32),
            pltpu.VMEM((NB, BLK), i32),
            pltpu.VMEM((2, HALF, EXT * BLK), bf16),
            pltpu.VMEM((HALF, NH * BLK), bf16),
            pltpu.VMEM((EXT, 32, BLK), bf16),
            pltpu.VMEM((NB, 4 * BLK, 2 * BLK), bf16),
            pltpu.VMEM((TILES, 3 * BLK, BLK), bf16),
            pltpu.VMEM((NB, 32, 2 * BLK), bf16),
            pltpu.VMEM((TILES * PITCH, BLK), f32),
            pltpu.VMEM((2 * HALF, TILES, BLK), bf16),
            pltpu.VMEM((PLANE * SRC_ROWS, TILES), bf16),
            pltpu.VMEM((2 * HALF, PLANE * SRC_ROWS, BLK), bf16),
            pltpu.VMEM((PLANE, 1, BLK), f32),
            pltpu.VMEM((HALF, 32 * SRC_ROWS, BLK), bf16),
            pltpu.VMEM((32, 1, BLK), f32),
            pltpu.VMEM((NZ * SLOTS, 32 * SRC_ROWS), bf16),
            pltpu.VMEM((HALF, NZ * SLOTS, BLK), bf16),
            pltpu.VMEM((HALF, SLOTS, BLK), f32),
            pltpu.VMEM((HALF, (NZ - 1) * SLOTS, BLK), bf16),
            pltpu.VMEM((16 * OPITCH, BLK), f32),
            pltpu.VMEM((PLANE * SRC_ROWS, TILES), bf16),
            pltpu.VMEM((2 * ZN, PLANE * SRC_ROWS, BLK), bf16),
            pltpu.VMEM((NZ, 1, BLK), f32),
            pltpu.VMEM((ZN, 32 * SRC_ROWS, BLK), bf16),
            pltpu.VMEM((2 * NZ, 1, BLK), f32),
            pltpu.VMEM((PLANE * SLOTS, 32 * SRC_ROWS), bf16),
            pltpu.VMEM((ZN, PLANE * SLOTS, BLK), bf16),
            pltpu.VMEM((ZN, SLOTS, BLK), f32),
            pltpu.VMEM((ZN, (PLANE - 1) * SLOTS, BLK), bf16),
            dma((6,)),
            dma,
            dma((8,)),
            dma((6,)),
            pltpu.SemaphoreType.REGULAR,
            pltpu.SemaphoreType.REGULAR,
            dma,
            dma,
            dma((CHUNKS,)),
            dma((CHUNKS,)),
            dma((CHUNKS,)),
            dma((CHUNKS,)),
            dma,
            dma,
            dma,
            dma,
            dma,
            dma,
        ],
        compiler_params=pltpu.CompilerParams(
            collective_id=0, has_side_effects=True, vmem_limit_bytes=48 * 1024 * 1024
        ),
    )(
        *(
            pltpu.with_memory_space_constraint(a, pltpu.HBM)
            for a in (
                ocean,
                grad_weight.reshape(NB, 4 * BLK, 2 * BLK),
                neighbours.T,
                remap_weight,
                tile_src[None, :],
                tile_atm[None, :],
                atm_owner.reshape(NB, BLK),
            )
        )
    )


def solution(mesh):
    in_specs = (
        P("field", "dom"),
        P("dom", None, None, None),
        P("dom", None),
        P(("dom", "field"), None, None),
        P(("dom", "field")),
        P(("dom", "field")),
        P(),
    )
    out_specs = P("field", "dom")
    return jax.shard_map(local, mesh=mesh, in_specs=in_specs, out_specs=out_specs, check_vma=False)
```
